32 devices in a mesh: swath: 2 (over x), band: 16 (over z, y, core).
Axes of the slice: x: 2, y: 2, z: 4, core: 2. Of those that a mesh axis runs over, the one named last changes fastest.
Arguments:
- design: bfloat16 [512, 16384], P(('swath', 'band')), parts along dimension 0, may hold values from 0 to 1
- row_taps: bfloat16 [8, 33], replicated, may hold values from -1 to 1
- column_taps: bfloat16 [8, 33], replicated, may hold values from -1 to 1
- kernel_weight: float32 [8], replicated, may hold values from 0.5 to 2
- interp: bfloat16 [32, 8], replicated, may hold values from 0 to 0.29882812
- block_shift: int32 [2, 4, 16], P(None, 'swath', 'band'), parts along dimension 1, may hold values from -24 to 24
- block_phase: int32 [2, 4, 16], P(None, 'swath', 'band'), parts along dimension 1, may hold values from 0 to 31
- care: int32 [4, 16], P('swath', 'band'), parts along dimension 0, may hold values 0 or 1
- image: bfloat16 [512, 16384], P('swath', 'band'), parts along dimension 0, may hold values from 0 to 20, as said below
Outputs:
- diff_map: bfloat16 [512, 16384], P('swath', 'band'), parts along dimension 0
The draws below stay inside these ranges and needn't reach their ends.
There are 2 independent parts, one for each index of `swath`. The reference program is written for one: setup_inputs(seed, part) draws one part's arguments, and reference() takes and returns one part's arrays. A program takes and returns all parts, laid end to end along the dimension named above; an argument that names none is the same for every part. Nothing has to cross between parts.
Inputs may be any that keep to these rules, and one draw needn't show every extreme that they name: `image`: nonnegative intensities.
All inputs are finite; a program needn't handle non-finite values. No bound on the sum of `care` on one device may be relied on, other than what follows from the above.
Results may differ from the reference program's by a relative error of at most 0.0045.
Values may be sent and summed in bfloat16 or wider, within the bound.
A program may use at most 64 MiB of HBM per device.

```python
import math
import jax
import jax.numpy as jnp
from jax import lax

W = 16384
NK = 8
KH = 16
SHIFT = 24
IH = 4
NF = 32
BLK = 128
P_SIZE = 28
H = 256
CW = 1024
BROWS = 2
N_BAND = 16


def draw_image(key, part):
    first = jax.random.fold_in(jax.random.fold_in(key, 7), 0)
    columns = jnp.arange(W, dtype=jnp.float32)
    ramp = 1.0 + 2.0 * columns / (W - 1)
    base = jax.random.uniform(first, (H, W), jnp.float32, 0.5, 1.5)
    return (base * ramp[None, :]).astype(jnp.bfloat16)


def with_ends(values, own_key, smallest, high):
    longest = values.shape.index(max(values.shape))
    spots = []
    for shift in (0, 1):
        where = [jax.random.randint(jax.random.fold_in(own_key, axis), (), 0, length) for axis, length in enumerate(values.shape)]
        where[longest] = (where[longest] + shift) % values.shape[longest]
        spots.append(tuple(where))
    return values.at[spots[0]].set(smallest).at[spots[1]].set(high)


def block_scale(rng, dims, shards, low, top_value):
    def one(dim, blocks):
        heights = jax.random.uniform(jax.random.fold_in(jax.random.fold_in(rng, 6), dim), (blocks,), jnp.float32, low / len(shards), top_value / len(shards))
        return jnp.repeat(jnp.exp(heights), dims[dim] // blocks).reshape((-1,) + (1,) * (len(dims) - dim - 1))

    level = one(*shards[0])
    for cut in shards[1:]:
        level = level * one(*cut)
    return level


def normal_values(rng, extent, width, bound, held_as=jnp.bfloat16):
    values = jax.random.normal(rng, extent, jnp.float32) * width
    return jnp.minimum(jnp.maximum(values, -bound), bound).astype(held_as)


def setup_inputs(seed: int = 0, part: int = 0) -> dict:
    arg_keys = jax.random.split(jax.random.key(seed), 10)
    part_splits = jax.random.split(jax.random.fold_in(arg_keys[9], part), 10)
    design = jnp.clip(1.0 * jax.random.uniform(part_splits[0], (H, W), jnp.float32) ** block_scale(part_splits[0], (H, W), ((0, 16),), -0.2, 0.2), 0.0, 1.0).astype(jnp.bfloat16)
    row_taps = normal_values(arg_keys[1], (NK, 2 * KH + 1), (2 * KH + 1) ** -0.5, 1.0)
    column_taps = normal_values(arg_keys[2], (NK, 2 * KH + 1), (2 * KH + 1) ** -0.5, 1.0)
    kernel_weight = jnp.clip(jnp.exp(jax.random.uniform(arg_keys[3], (NK,), jnp.float32, math.log(0.5), math.log(2.0))), 0.5, 2.0)
    interp = jnp.clip(jax.random.uniform(arg_keys[4], (NF, 2 * IH), jnp.float32, 0.0, 0.29882812), 0.0, 0.29882812).astype(jnp.bfloat16)
    block_shift = with_ends(jax.random.randint(part_splits[5], (2, BROWS, N_BAND), -SHIFT, SHIFT + 1), jax.random.fold_in(part_splits[5], 1), -SHIFT, SHIFT).astype(jnp.int32)
    block_phase = with_ends(jax.random.randint(part_splits[6], (2, BROWS, N_BAND), 0, NF), jax.random.fold_in(part_splits[6], 1), 0, NF - 1).astype(jnp.int32)
    care = with_ends((jax.random.randint(part_splits[7], (BROWS, N_BAND), 0, 3) < 2).astype(jnp.int32), jax.random.fold_in(part_splits[7], 1), 0, 1)
    image = draw_image(jax.random.fold_in(jax.random.fold_in(arg_keys[9], part), 71), part)
    return {"design": design, "row_taps": row_taps, "column_taps": column_taps, "kernel_weight": kernel_weight, "interp": interp, "block_shift": block_shift, "block_phase": block_phase, "care": care, "image": image}


epsilon = 1e-05

def band_matrix(offsets, phases, interp, size_out, size_in):
    table = jax.nn.one_hot(phases, NF, dtype=jnp.float32)
    weights = jnp.dot(table, interp.astype(jnp.float32), precision=lax.Precision.HIGHEST)
    outer = jnp.arange(size_out, dtype=jnp.int32)
    inner = jnp.arange(size_in, dtype=jnp.int32)
    position = inner[None, None, :] - outer[None, :, None] - offsets[:, None, None] + (IH - 1 - P_SIZE)
    matrix = jnp.zeros(position.shape, jnp.float32)
    for tap in range(2 * IH):
        matrix = matrix + jnp.where(position == tap, weights[:, tap][:, None, None], 0.0)
    return matrix.astype(jnp.bfloat16)

def warp_strip(framed, shifts, phases, interp):
    height = framed.shape[0] - BLK - 2 * P_SIZE
    across = framed.shape[1]
    strip_cols = across - 2 * P_SIZE
    count = height // BLK
    upper = framed[:height].reshape(count, BLK, across)[:, :P_SIZE]
    middle = framed[P_SIZE:P_SIZE + height].reshape(count, BLK, across)
    lower = framed[BLK + P_SIZE:BLK + P_SIZE + height].reshape(count, BLK, across)[:, :P_SIZE]
    blocks = jnp.concatenate([upper, middle, lower], axis=1)
    row_matrix = band_matrix(shifts[0], phases[0], interp, BLK, BLK + 2 * P_SIZE)
    column_matrix = band_matrix(shifts[1], phases[1], interp, strip_cols, across)
    partial_value = jnp.einsum('brs,bsc->brc', row_matrix.astype(jnp.float32), blocks.astype(jnp.float32), precision=lax.Precision.HIGHEST).astype(jnp.bfloat16)
    return jnp.einsum('brs,bcs->brc', partial_value.astype(jnp.float32), column_matrix.astype(jnp.float32), precision=lax.Precision.HIGHEST)

def finish(warped, strip, cares):
    count, rows, cols = warped.shape
    measured = strip.reshape(count, rows, cols).astype(jnp.float32)
    difference = (cares.astype(jnp.float32)[:, None, None] * (measured - warped)).reshape(count * rows, cols)
    padded = jnp.pad(difference, ((1, 1), (0, 0)))
    return difference + 0.5 * (padded[:-2] + padded[2:])

def reference(design, row_taps, column_taps, kernel_weight, interp, block_shift, block_phase, care, image):
    plane = design.astype(jnp.float32)[None, None]

    def add_kernel(kernel, total):
        row_filter = row_taps[kernel].astype(jnp.float32).reshape(1, 1, 2 * KH + 1, 1)
        smoothed = lax.conv_general_dilated(plane, row_filter, (1, 1), ((KH, KH), (0, 0)), precision=lax.Precision.HIGHEST).astype(jnp.bfloat16)
        column_filter = column_taps[kernel].astype(jnp.float32).reshape(1, 1, 1, 2 * KH + 1)
        field = lax.conv_general_dilated(smoothed.astype(jnp.float32), column_filter, (1, 1), ((0, 0), (KH, KH)), precision=lax.Precision.HIGHEST)[0, 0]
        return total + kernel_weight[kernel] * field * field
    total = lax.fori_loop(0, NK, add_kernel, jnp.zeros((H, W), jnp.float32))
    intensity = total.astype(jnp.bfloat16)
    padded = jnp.pad(intensity, ((P_SIZE, BLK + P_SIZE), (P_SIZE, P_SIZE)))
    strips = image.reshape(H, N_BAND, CW).transpose(1, 0, 2)
    starts = (jnp.arange(N_BAND, dtype=jnp.int32) * CW).astype(jnp.int32)

    def one_strip(items):
        start, shifts, phases, cares, strip = items
        framed = lax.dynamic_slice_in_dim(padded, start, CW + 2 * P_SIZE, axis=1)
        warped = warp_strip(framed, shifts, phases, interp)
        return finish(warped, strip, cares)
    filtered = lax.map(one_strip, (starts, jnp.moveaxis(block_shift, 2, 0), jnp.moveaxis(block_phase, 2, 0), care.T, strips))
    cells = H * W
    mean = jnp.sum(filtered) / cells
    variance = jnp.sum((filtered - mean) * (filtered - mean)) / cells
    care_rows = jnp.repeat(care.T.astype(jnp.float32), BLK, axis=1)
    result = care_rows[:, :, None] * (filtered - mean) * lax.rsqrt(variance + epsilon)
    return result.transpose(1, 0, 2).reshape(H, W).astype(jnp.bfloat16)
```

```python
import functools

import jax
import jax.numpy as jnp
from jax import lax
from jax.experimental import pallas as pl
from jax.experimental.pallas import tpu as pltpu
from jax.sharding import PartitionSpec as P

NK = 8
KH = 16
IH = 4
BLK = 128
P_SIZE = 28
LANES = 128
HALF = LANES // 2
EDGE = 32
UNIT = 128
LEVELS = 4
REACH = 2 * KH + 1
LEAD = P_SIZE + KH
INNER = LANES - LEAD

epsilon = 1e-05

F32 = jnp.float32
BF16 = jnp.bfloat16


def pin(x):
    return pltpu.with_memory_space_constraint(x, pltpu.HBM)


def skewed(row, rows):
    base = jnp.broadcast_to(row, (rows, row.shape[1]))
    return pltpu.roll(base, 0, 1, stride=1, stride_axis=0)


def split(total):
    return [min(UNIT, total - at) for at in range(0, total, UNIT)]


def plan(tiles):
    if tiles < 4:
        return [[(0, tiles)]]
    events = [[(0, 1), (tiles - 1, 1)]]
    low, high = 1, tiles - 2
    left = True
    while low <= high:
        span = min(2, high - low + 1)
        events.append([(low if left else high - span + 1, span)])
        low, high = (low + span, high) if left else (low, high - span)
        left = not left
    return events


def kernel(
    n, height, width,
    weight_hbm, shift_hbm, phase_hbm, care_hbm,
    design_hbm, row_hbm, column_hbm, interp_hbm, image_hbm,
    filt, mean_ref, scale_ref,
    weight_ref, shift_ref, phase_ref, care_ref,
    row_ref, column_ref, interp_ref,
    recv, before, after, ends, image, row_mats, column_mats, outer_mats,
    warp_rows, warp_columns, warp_last, smooth, intensity, partial,
    diff, partial_sums, stats_mine, stats_all,
    send_sem, recv_sem, relay_send, relay_recv, stat_send, stat_recv, load_sem,
):
    me = lax.axis_index("band")
    rows = height // n
    strip = width // n
    tiles = strip // LANES
    level_rows = height // LEVELS
    half_rows = 2 * level_rows
    count = height // BLK
    events = plan(tiles)
    pieces_of = [(e, lo, span) for e, event in enumerate(events) for lo, span in event]

    barrier = pltpu.get_barrier_semaphore()

    def greet(i, carry):
        peer = lax.rem(me + i, n)
        pl.semaphore_signal(
            barrier, inc=1, device_id={"band": peer}, device_id_type=pl.DeviceIdType.MESH
        )
        return carry

    lax.fori_loop(1, n, greet, 0)

    mine = pl.ds(pl.multiple_of(KH + me * rows, rows), rows)
    loads = [
        pltpu.make_async_copy(source, target, load_sem.at[i])
        for i, (source, target) in enumerate(
            [
                (row_hbm, row_ref),
                (column_hbm, column_ref),
                (interp_hbm, interp_ref),
                (weight_hbm, weight_ref),
                (shift_hbm, shift_ref),
                (phase_hbm, phase_ref),
                (care_hbm, care_ref),
                (image_hbm, image),
                (
                    design_hbm.at[:, pl.ds(pl.multiple_of(me * strip, LANES), strip)],
                    recv.at[mine, :],
                ),
            ]
        )
    ]
    for load in loads:
        load.start()

    flips = {}
    bit = 1
    while bit < n:
        flips[bit] = bit * (1 - 2 * lax.rem(me // bit, 2))
        bit *= 2

    def partner(i):
        return me + sum(flip for bit, flip in flips.items() if i & bit)

    def send(peer, slot, lo, span):
        pltpu.make_async_remote_copy(
            src_ref=design_hbm.at[
                :, pl.ds(pl.multiple_of(peer * strip + lo * LANES, LANES), span * LANES)
            ],
            dst_ref=recv.at[mine, pl.ds(lo * LANES, span * LANES)],
            send_sem=send_sem.at[slot],
            recv_sem=recv_sem.at[slot],
            device_id={"band": peer},
            device_id_type=pl.DeviceIdType.MESH,
        ).start()

    def block(extent, columns):
        return recv.at[pl.ds(0, extent), pl.ds(0, columns)]

    def settle(sem, extent, columns):
        pltpu.make_async_copy(block(extent, columns), block(extent, columns), sem).wait()

    sizes = [(half_rows - rows, strip), (level_rows, strip)] + [
        (level_rows, sum(span for _, span in event) * LANES) for event in events
    ]

    pl.semaphore_wait(barrier, n - 1)
    for i in range(1, n // 2):
        send(partner(i), 0, 0, tiles)
    for i in range(n // 2, 3 * n // 4):
        send(partner(i), 1, 0, tiles)
    for e, lo, span in pieces_of:
        for i in range(3 * n // 4, n):
            send(partner(i), 2 + e, lo, span)

    level = me // (n // LEVELS)
    second = lax.rem(level + 2, LEVELS)
    third = LEVELS - 1 - level
    upper = level // 2

    def by_level(*values):
        out = jnp.int32(values[0])
        for i in range(1, LEVELS):
            out = jnp.where(level == i, values[i], out)
        return pl.multiple_of(out, KH)

    first_rows = half_rows - KH
    second_rows = level_rows - KH
    third_rows = level_rows + 2 * KH
    first_start = by_level(0, 0, half_rows + KH, half_rows + KH)
    second_start = by_level(
        half_rows - KH, height - second_rows, 0, half_rows + KH - second_rows
    )
    third_start = by_level(
        height - third_rows, half_rows - KH, half_rows + KH - third_rows, 0
    )

    zero_rows = jnp.zeros((KH, LANES), BF16)
    for edge in (before, after):
        edge[:KH, :] = zero_rows
        edge[KH + height :, :] = zero_rows
    recv[:KH, :] = jnp.zeros((KH, strip), BF16)
    recv[KH + height :, :] = jnp.zeros((KH, strip), BF16)

    @pl.when(me == 0)
    def _():
        before[KH : KH + height, :] = jnp.zeros((height, LANES), BF16)

    @pl.when(me == n - 1)
    def _():
        after[KH : KH + height, :] = jnp.zeros((height, LANES), BF16)

    wide = strip + LANES
    intensity[:EDGE, :] = jnp.zeros((EDGE, wide), BF16)
    intensity[EDGE + height :, :] = jnp.zeros((EDGE, wide), BF16)
    diff[:8, :] = jnp.zeros((8, strip), F32)
    diff[8 + height :, :] = jnp.zeros((8, strip), F32)
    partial_sums[...] = jnp.zeros((16, LANES), F32)

    for load in loads[:-2]:
        load.wait()

    pad = jnp.zeros((NK, LANES - REACH), F32)
    row_table = jnp.concatenate([row_ref[...].astype(F32), pad, jnp.zeros((NK, LANES), F32)], axis=1)
    column_table = jnp.concatenate([column_ref[...].astype(F32), pad], axis=1)
    from_lane = lax.broadcasted_iota(jnp.int32, (LANES, LANES), 0)
    to_lane = lax.broadcasted_iota(jnp.int32, (LANES, LANES), 1)
    turned = jnp.where(lax.rem(2 * LANES - INNER - to_lane, LANES) == from_lane, 1.0, 0.0)
    backward = jnp.dot(
        column_table.astype(BF16), turned.astype(BF16), preferred_element_type=F32
    )
    backward_half = pltpu.roll(backward, HALF, 1)
    square = (2 * LANES, LANES)
    down = lax.broadcasted_iota(jnp.int32, square, 0)
    across = lax.broadcasted_iota(jnp.int32, square, 1)
    place = down - across - INNER
    inside = jnp.logical_and(place >= 0, place < REACH)
    low_lane = across < HALF
    place_far = lax.rem(down - across - INNER - HALF + 4 * LANES, 2 * LANES)
    inside_outer = jnp.where(low_lane, jnp.where(inside, 1, 0), jnp.where(place_far < REACH, 1, 0)) > 0
    for k in range(NK):
        row_mats[k * UNIT : (k + 1) * UNIT, :] = skewed(row_table[k : k + 1], UNIT).astype(BF16)
        near = skewed(backward[k : k + 1], 2 * LANES)
        far = skewed(backward_half[k : k + 1], 2 * LANES)
        column_mats[k] = jnp.where(inside, near, 0.0).astype(BF16)
        outer_mats[k] = jnp.where(
            inside_outer, jnp.where(low_lane, near, far), 0.0
        ).astype(BF16)

    table = interp_ref[...].astype(F32)
    phases = lax.broadcasted_iota(jnp.int32, table.shape, 1)
    lane_wide = lax.broadcasted_iota(jnp.int32, (1, 2 * LANES), 1)
    lane_one = lax.broadcasted_iota(jnp.int32, (1, LANES), 1)

    def chosen(phase):
        row = jnp.sum(jnp.where(phases == phase, table, 0.0), axis=1, keepdims=True)
        return [row[t : t + 1] for t in range(2 * IH)]

    for b in range(count):
        u = chosen(phase_ref[0, 0, b])
        v = chosen(phase_ref[1, 0, b])
        lead = EDGE + 1 - IH + shift_ref[0, 0, b]
        row = jnp.zeros((1, 2 * LANES), F32)
        for tap in range(2 * IH):
            row = jnp.where(lane_wide == lead + tap, u[tap], row)
        warp_rows[b] = skewed(row, BLK).astype(BF16)
        lead = P_SIZE + 1 - IH + shift_ref[1, 0, b]
        row = jnp.zeros((1, LANES), F32)
        for tap in range(2 * IH):
            row = jnp.where(lane_one == LANES - lead - tap, v[tap], row)
        steep = skewed(row, 2 * LANES)
        spot = down - across - lead
        matrix = jnp.where(jnp.logical_and(spot >= 0, spot < 2 * IH), steep, 0.0)
        warp_columns[b] = matrix.astype(BF16)
        warp_last[b, :LANES, :] = matrix[:LANES].astype(BF16)
        warp_last[b, LANES : LANES + HALF, :] = jnp.zeros((HALF, LANES), BF16)
        warp_last[b, LANES + HALF :, :] = matrix[LANES : LANES + HALF].astype(BF16)

    def relay(stage, peer, side, start, extent):
        span = pl.ds(pl.multiple_of(KH + start, KH), extent)
        source = recv.at[span, pl.ds(0, LANES)] if side == 0 else recv.at[
            span, pl.ds(strip - LANES, LANES)
        ]
        target = after.at[span, :] if side == 0 else before.at[span, :]
        return pltpu.make_async_remote_copy(
            src_ref=source,
            dst_ref=target,
            send_sem=relay_send.at[stage, side],
            recv_sem=relay_recv.at[stage, side],
            device_id={"band": peer},
            device_id_type=pl.DeviceIdType.MESH,
        )

    relays = [
        (upper * half_rows, half_rows),
        (second * level_rows, level_rows),
        (third * level_rows, level_rows),
    ]

    def pass_on(stage):
        @pl.when(me > 0)
        def _():
            relay(stage, me - 1, 0, *relays[stage]).start()

        @pl.when(me < n - 1)
        def _():
            relay(stage, me + 1, 1, *relays[stage]).start()

    def take_ends():
        for stage, (_, extent) in enumerate(relays):
            region = block(extent, LANES)

            @pl.when(me < n - 1)
            def _():
                pltpu.make_async_copy(region, region, relay_recv.at[stage, 0]).wait()

            @pl.when(me > 0)
            def _():
                pltpu.make_async_copy(region, region, relay_recv.at[stage, 1]).wait()

    def finish_relays():
        for stage, (_, extent) in enumerate(relays):
            region = block(extent, LANES)

            @pl.when(me > 0)
            def _():
                pltpu.make_async_copy(region, region, relay_send.at[stage, 0]).wait()

            @pl.when(me < n - 1)
            def _():
                pltpu.make_async_copy(region, region, relay_send.at[stage, 1]).wait()

    def row_kernels(extent):
        return jnp.concatenate(
            [row_mats[k * UNIT : k * UNIT + extent, : extent + 2 * KH] for k in range(NK)], axis=0
        )

    def smear(start, extent, at, lo, span):
        window = recv[
            pl.ds(pl.multiple_of(start, KH), extent + 2 * KH), lo * LANES : (lo + span) * LANES
        ]
        smooth[at : at + NK * extent, lo * LANES : (lo + span) * LANES] = jnp.dot(
            row_kernels(extent), window, preferred_element_type=F32
        ).astype(BF16)

    def render(start, extent, at, panels):
        into = pl.multiple_of(EDGE + start, KH)
        total = jnp.zeros((len(panels) * extent, LANES), F32)
        for k in range(NK):
            pieces = []
            for p in panels:
                own = pl.ds(at + k * extent, extent)
                if p == 0:
                    piece = smooth[own, :LANES]
                    pieces.append(jnp.concatenate([piece, piece], axis=1))
                else:
                    pieces.append(smooth[own, (p - 1) * LANES : (p + 1) * LANES])
            field = jnp.dot(
                jnp.concatenate(pieces, axis=0), column_mats[k], preferred_element_type=F32
            )
            total = total + weight_ref[k] * field * field
        for i, p in enumerate(panels):
            intensity[pl.ds(into, extent), p * LANES : (p + 1) * LANES] = total[
                i * extent : (i + 1) * extent
            ].astype(BF16)

    def render_outer():
        lane = lax.broadcasted_iota(jnp.int32, (height + 2 * KH, LANES), 1) < HALF
        ends[:, :LANES] = jnp.where(lane, after[...], before[...])
        ends[:, LANES:] = jnp.where(lane, recv[:, :LANES], recv[:, strip - LANES :])
        start = 0
        for extent in split(height):
            lanes = lax.broadcasted_iota(jnp.int32, (extent, LANES), 1)
            spread = jnp.dot(
                row_kernels(extent), ends[start : start + extent + 2 * KH, :],
                preferred_element_type=F32,
            ).astype(BF16)
            total = jnp.zeros((extent, LANES), F32)
            for k in range(NK):
                field = jnp.dot(
                    spread[k * extent : (k + 1) * extent], outer_mats[k],
                    preferred_element_type=F32,
                )
                total = total + weight_ref[k] * field * field
            left = lanes < HALF
            column = jnp.where(left, me * strip + lanes, me * strip + strip + lanes - HALF) - P_SIZE
            total = jnp.where(jnp.logical_and(column >= 0, column < width), total, 0.0).astype(BF16)
            into = slice(EDGE + start, EDGE + start + extent)
            intensity[into, strip:] = total
            intensity[into, :LANES] = jnp.where(lanes < LEAD, total, intensity[into, :LANES])
            start += extent

    def halfway(panels):
        runs = []
        for p in sorted(panels):
            if runs and runs[-1][1] == p:
                runs[-1][1] = p + 1
            else:
                runs.append([p, p + 1])
        for b in range(count):
            for lo, hi in runs:
                partial[b * BLK : (b + 1) * BLK, lo * LANES : hi * LANES] = jnp.dot(
                    warp_rows[b, :, : BLK + 2 * EDGE],
                    intensity[b * BLK : (b + 1) * BLK + 2 * EDGE, lo * LANES : hi * LANES],
                    preferred_element_type=F32,
                ).astype(BF16)

    def finish(targets):
        targets = sorted(targets)
        common = [q for q in targets if q < tiles - 1]
        for b in range(count):
            own = slice(b * BLK, (b + 1) * BLK)
            care = care_ref[0, b].astype(F32)
            results = []
            if common:
                warped = jnp.dot(
                    jnp.concatenate(
                        [partial[own, q * LANES : (q + 2) * LANES] for q in common], axis=0
                    ),
                    warp_columns[b],
                    preferred_element_type=F32,
                )
                results += [(q, warped[i * BLK : (i + 1) * BLK]) for i, q in enumerate(common)]
            if tiles - 1 in targets:
                q = tiles - 1
                results.append(
                    (
                        q,
                        jnp.dot(
                            partial[own, q * LANES : (q + 2) * LANES], warp_last[b],
                            preferred_element_type=F32,
                        ),
                    )
                )
            for q, warped in results:
                measured = image[own, q * LANES : (q + 1) * LANES].astype(F32)
                diff[8 + b * BLK : 8 + (b + 1) * BLK, q * LANES : (q + 1) * LANES] = care * (
                    measured - warped
                )
        first = partial_sums[:8, :]
        second = partial_sums[8:, :]
        for q in targets:
            column = slice(q * LANES, (q + 1) * LANES)
            for start in range(0, height, BLK):
                around = diff[start : start + BLK + 16, column]
                value = around[8 : 8 + BLK] + 0.5 * (around[7 : 7 + BLK] + around[9 : 9 + BLK])
                filt[start : start + BLK, column] = value
                power = value * value
                for r in range(0, BLK, 8):
                    first = first + value[r : r + 8]
                    second = second + power[r : r + 8]
        partial_sums[:8, :] = first
        partial_sums[8:, :] = second

    def whole(start, total):
        at = 0
        for extent in split(total):
            smear(start + at, extent, 0, 0, tiles)
            for p in range(0, tiles, 4):
                render(start + at, extent, 0, list(range(p, min(p + 4, tiles))))
            at += extent

    loads[-1].wait()
    settle(recv_sem.at[0], *sizes[0])
    pass_on(0)
    whole(first_start, first_rows)
    settle(recv_sem.at[1], *sizes[1])
    pass_on(1)
    whole(second_start, second_rows)
    loads[-2].wait()

    seen, drawn, halves, done = set(), set(), set(), set()
    for e, event in enumerate(events):
        settle(recv_sem.at[2 + e], *sizes[2 + e])
        if e == 0:
            pass_on(2)
        for lo, span in event:
            seen.update(range(lo, lo + span))
        fresh = [
            p for p in range(tiles)
            if p in seen and (p == 0 or p - 1 in seen) and p not in drawn
        ]
        drawn.update(fresh)
        at = 0
        for extent in split(third_rows):
            for lo, span in event:
                smear(third_start + at, extent, NK * at, lo, span)
            if fresh:
                render(third_start + at, extent, NK * at, fresh)
            at += extent
        if e == max(len(events) - 2, 0):
            take_ends()
            render_outer()
            drawn.add(tiles)
        if tiles in drawn:
            ready = drawn - halves
            halfway(ready)
            halves.update(ready)
            targets = {q for q in range(tiles) if q in halves and q + 1 in halves} - done
            finish(targets)
            done.update(targets)

    stats_mine[0:1, :] = jnp.sum(partial_sums[:8, :], axis=0, keepdims=True)
    stats_mine[1:2, :] = jnp.sum(partial_sums[8:, :], axis=0, keepdims=True)

    def stat_to(peer):
        return pltpu.make_async_remote_copy(
            src_ref=stats_mine,
            dst_ref=stats_all.at[me],
            send_sem=stat_send.at[peer],
            recv_sem=stat_recv.at[me],
            device_id={"band": peer},
            device_id_type=pl.DeviceIdType.MESH,
        )

    def stat_from(peer):
        return pltpu.make_async_remote_copy(
            src_ref=stats_mine,
            dst_ref=stats_all.at[peer],
            send_sem=stat_send.at[peer],
            recv_sem=stat_recv.at[peer],
            device_id={"band": peer},
            device_id_type=pl.DeviceIdType.MESH,
        )

    def send_stats(i, carry):
        peer = lax.rem(me + n // 2 + i, n)

        @pl.when(peer != me)
        def _():
            stat_to(peer).start()

        return carry

    lax.fori_loop(0, n, send_stats, 0)
    stats_all[me] = stats_mine[...]

    for slot, size in enumerate(sizes):
        settle(send_sem.at[slot], *size)
    finish_relays()

    def take_stats(i, carry):
        peer = lax.rem(me + i, n)
        stat_from(peer).wait_recv()
        stat_to(peer).wait_send()
        return carry

    lax.fori_loop(1, n, take_stats, 0)

    sums = lax.fori_loop(
        0, n, lambda i, carry: carry + stats_all[i], jnp.zeros((2, LANES), F32)
    )
    cells = height * width
    mean = jnp.sum(sums[0:1], axis=1, keepdims=True) / cells
    power = jnp.sum(sums[1:2], axis=1, keepdims=True) / cells
    scale = lax.rsqrt(power - mean * mean + epsilon)
    mean_ref[...] = jnp.broadcast_to(mean, (1, strip))
    for b in range(count):
        scale_ref[b : b + 1, :] = jnp.broadcast_to(care_ref[0, b].astype(F32) * scale, (1, strip))


def on_device(
    design, row_taps, column_taps, kernel_weight, interp, block_shift, block_phase, care, image
):
    n = lax.axis_size("band")
    rows, width = design.shape
    height, strip = image.shape
    wide = strip + LANES
    count = height // BLK
    slots = 2 + len(plan(strip // LANES))
    tall = height + 2 * KH
    hbm = pl.BlockSpec(memory_space=pltpu.HBM)
    vmem = pl.BlockSpec(memory_space=pltpu.VMEM)
    filtered, mean, scale = pl.pallas_call(
        functools.partial(kernel, n, height, width),
        out_shape=(
            jax.ShapeDtypeStruct((height, strip), F32),
            jax.ShapeDtypeStruct((1, strip), F32),
            jax.ShapeDtypeStruct((count, strip), F32),
        ),
        in_specs=[hbm] * 9,
        out_specs=(vmem, vmem, vmem),
        scratch_shapes=[
            pltpu.SMEM((NK,), F32),
            pltpu.SMEM((2, 1, count), jnp.int32),
            pltpu.SMEM((2, 1, count), jnp.int32),
            pltpu.SMEM((1, count), jnp.int32),
            pltpu.VMEM(row_taps.shape, BF16),
            pltpu.VMEM(column_taps.shape, BF16),
            pltpu.VMEM(interp.shape[::-1], BF16),
            pltpu.VMEM((tall, strip), BF16),
            pltpu.VMEM((tall, LANES), BF16),
            pltpu.VMEM((tall, LANES), BF16),
            pltpu.VMEM((tall, 2 * LANES), BF16),
            pltpu.VMEM((height, strip), BF16),
            pltpu.VMEM((NK * UNIT, 2 * LANES), BF16),
            pltpu.VMEM((NK, 2 * LANES, LANES), BF16),
            pltpu.VMEM((NK, 2 * LANES, LANES), BF16),
            pltpu.VMEM((count, BLK, 2 * LANES), BF16),
            pltpu.VMEM((count, 2 * LANES, LANES), BF16),
            pltpu.VMEM((count, 2 * LANES, LANES), BF16),
            pltpu.VMEM((NK * max(UNIT, height // LEVELS + 2 * KH), strip), BF16),
            pltpu.VMEM((height + 2 * EDGE, wide), BF16),
            pltpu.VMEM((height, wide), BF16),
            pltpu.VMEM((height + 16, strip), F32),
            pltpu.VMEM((16, LANES), F32),
            pltpu.VMEM((2, LANES), F32),
            pltpu.VMEM((n, 2, LANES), F32),
            pltpu.SemaphoreType.DMA((slots,)),
            pltpu.SemaphoreType.DMA((slots,)),
            pltpu.SemaphoreType.DMA((3, 2)),
            pltpu.SemaphoreType.DMA((3, 2)),
            pltpu.SemaphoreType.DMA((n,)),
            pltpu.SemaphoreType.DMA((n,)),
            pltpu.SemaphoreType.DMA((9,)),
        ],
        compiler_params=pltpu.CompilerParams(
            collective_id=0, has_side_effects=True, vmem_limit_bytes=48 * 1024 * 1024
        ),
    )(
        pin(kernel_weight),
        pin(jnp.transpose(block_shift, (0, 2, 1))),
        pin(jnp.transpose(block_phase, (0, 2, 1))),
        pin(care.T),
        pin(design),
        pin(row_taps),
        pin(column_taps),
        pin(interp.T),
        pin(image),
    )
    blocks = filtered.reshape(count, BLK, strip)
    out = (blocks - mean[:, None]) * scale[:, None]
    return out.reshape(height, strip).astype(BF16)


def solution(mesh):
    placed = (
        P(("swath", "band"), None),
        P(),
        P(),
        P(),
        P(),
        P(None, "swath", "band"),
        P(None, "swath", "band"),
        P("swath", "band"),
        P("swath", "band"),
    )
    return jax.shard_map(
        on_device, mesh=mesh, in_specs=placed, out_specs=P("swath", "band"), check_vma=False
    )
```

```python
import functools

import jax
import jax.numpy as jnp
from jax import lax
from jax.experimental import pallas as pl
from jax.experimental.pallas import tpu as pltpu
from jax.sharding import PartitionSpec as P

NK = 8
KH = 16
IH = 4
BLK = 128
P_SIZE = 28
LANES = 128
HALF = LANES // 2
EDGE = 32
UNIT = 128
REACH = 2 * KH + 1
LEAD = P_SIZE + KH
INNER = LANES - LEAD

LEVELS = 4
INNER_SENDS = {3: 0}
OUTER_SENDS = {3: 0}

epsilon = 1e-05

F32 = jnp.float32
BF16 = jnp.bfloat16


def pin(x):
    return pltpu.with_memory_space_constraint(x, pltpu.HBM)


def skewed(row, rows):
    base = jnp.broadcast_to(row, (rows, row.shape[1]))
    return pltpu.roll(base, 0, 1, stride=1, stride_axis=0)


def split(total):
    return [min(UNIT, total - at) for at in range(0, total, UNIT)]


def plan(tiles):
    if tiles < 4:
        return [[(0, tiles)]]
    events = [[(0, 1), (tiles - 1, 1)]]
    low, high = 1, tiles - 2
    left = True
    while low <= high:
        span = min(2, high - low + 1)
        events.append([(low if left else high - span + 1, span)])
        low, high = (low + span, high) if left else (low, high - span)
        left = not left
    return events


def kernel(
    n, height, width,
    weight_hbm, shift_hbm, phase_hbm, care_hbm,
    design_hbm, row_hbm, column_hbm, interp_hbm, image_hbm,
    filt, mean_ref, scale_ref,
    weight_ref, shift_ref, phase_ref, care_ref,
    row_ref, column_ref, interp_ref,
    recv, before, after, ends, image, row_mats, column_mats, outer_mats,
    warp_rows, warp_columns, warp_last, crossed, intensity, partial,
    diff, partial_sums, stats_mine, stats_all,
    send_sem, recv_sem, relay_send, relay_recv, end_send, end_recv, end_load, stat_send, stat_recv, load_sem,
):
    me = lax.axis_index("band")
    rows = height // n
    strip = width // n
    tiles = strip // LANES
    tall = height + 2 * KH
    count = height // BLK
    events = plan(tiles)

    barrier = pltpu.get_barrier_semaphore()

    def greet(i, carry):
        peer = lax.rem(me + i, n)
        pl.semaphore_signal(
            barrier, inc=1, device_id={"band": peer}, device_id_type=pl.DeviceIdType.MESH
        )
        return carry

    lax.fori_loop(1, n, greet, 0)

    mine = pl.ds(pl.multiple_of(KH + me * rows, rows), rows)
    loads = [
        pltpu.make_async_copy(source, target, load_sem.at[i])
        for i, (source, target) in enumerate(
            [
                (row_hbm, row_ref),
                (column_hbm, column_ref),
                (interp_hbm, interp_ref),
                (weight_hbm, weight_ref),
                (shift_hbm, shift_ref),
                (phase_hbm, phase_ref),
                (care_hbm, care_ref),
                (image_hbm, image),
                (
                    design_hbm.at[:, pl.ds(pl.multiple_of(me * strip, LANES), strip)],
                    recv.at[mine, :],
                ),
            ]
        )
    ]
    for load in loads:
        load.start()

    flips = {}
    bit = 1
    while bit < n:
        flips[bit] = bit * (1 - 2 * lax.rem(me // bit, 2))
        bit *= 2

    def partner(i):
        return me + sum(flip for bit, flip in flips.items() if i & bit)

    def send(peer, slot, lo, span):
        pltpu.make_async_remote_copy(
            src_ref=design_hbm.at[
                :, pl.ds(pl.multiple_of(peer * strip + lo * LANES, LANES), span * LANES)
            ],
            dst_ref=recv.at[mine, pl.ds(lo * LANES, span * LANES)],
            send_sem=send_sem.at[slot],
            recv_sem=recv_sem.at[slot],
            device_id={"band": peer},
            device_id_type=pl.DeviceIdType.MESH,
        ).start()

    def send_ends():
        for target, edge, tile in ((n // 2, before, -1), (n // 2 - 1, after, 0)):
            source = design_hbm.at[:, pl.ds((n // 2) * strip + tile * LANES, LANES)]
            place = edge.at[mine, :]

            @pl.when(me != target)
            def _():
                pltpu.make_async_remote_copy(
                    src_ref=source,
                    dst_ref=place,
                    send_sem=end_send.at[-tile],
                    recv_sem=end_recv,
                    device_id={"band": jnp.int32(target)},
                    device_id_type=pl.DeviceIdType.MESH,
                ).start()

            @pl.when(me == target)
            def _():
                pltpu.make_async_copy(source, place, end_load).start()

    def block(extent, columns):
        return recv.at[pl.ds(0, extent), pl.ds(0, columns)]

    def settle(sem, extent, columns):
        pltpu.make_async_copy(block(extent, columns), block(extent, columns), sem).wait()

    sizes = [(height - rows, sum(span for _, span in event) * LANES) for event in events]

    pl.semaphore_wait(barrier, n - 1)

    def send_pieces(chosen_events):
        for e in chosen_events:
            for i in range(1, n):
                for lo, span in events[e]:
                    send(partner(i), e, lo, span)

    def send_after(e):
        for mine_too, schedule in ((True, INNER_SENDS), (False, OUTER_SENDS)):
            batch = [x for x in range(1, len(events)) if schedule.get(x, -1) == e]
            if batch:
                @pl.when(inner == mine_too)
                def _():
                    send_pieces(batch)

    level = me // (n // LEVELS)
    inner = jnp.logical_and(level > 0, level < LEVELS - 1)
    send_pieces([0])
    send_ends()
    send_after(-1)

    zero_rows = jnp.zeros((KH, LANES), BF16)
    for edge in (before, after):
        edge[:KH, :] = zero_rows
        edge[KH + height :, :] = zero_rows
    recv[:KH, :] = jnp.zeros((KH, strip), BF16)
    recv[KH + height :, :] = jnp.zeros((KH, strip), BF16)

    @pl.when(me == 0)
    def _():
        before[KH : KH + height, :] = jnp.zeros((height, LANES), BF16)

    @pl.when(me == n - 1)
    def _():
        after[KH : KH + height, :] = jnp.zeros((height, LANES), BF16)

    wide = strip + LANES
    intensity[:EDGE, :] = jnp.zeros((EDGE, wide), BF16)
    intensity[EDGE + height :, :] = jnp.zeros((EDGE, wide), BF16)
    diff[:8, :] = jnp.zeros((8, strip), F32)
    diff[8 + height :, :] = jnp.zeros((8, strip), F32)
    partial_sums[...] = jnp.zeros((16, LANES), F32)

    for load in loads[:-2]:
        load.wait()

    pad = jnp.zeros((NK, LANES - REACH), F32)
    row_table = jnp.concatenate([row_ref[...].astype(F32), pad, jnp.zeros((NK, LANES), F32)], axis=1)
    column_table = jnp.concatenate([column_ref[...].astype(F32), pad], axis=1)
    from_lane = lax.broadcasted_iota(jnp.int32, (LANES, LANES), 0)
    to_lane = lax.broadcasted_iota(jnp.int32, (LANES, LANES), 1)
    turned = jnp.where(lax.rem(2 * LANES - INNER - to_lane, LANES) == from_lane, 1.0, 0.0)
    backward = jnp.dot(
        column_table.astype(BF16), turned.astype(BF16), preferred_element_type=F32
    )
    backward_half = pltpu.roll(backward, HALF, 1)
    square = (2 * LANES, LANES)
    down = lax.broadcasted_iota(jnp.int32, square, 0)
    across = lax.broadcasted_iota(jnp.int32, square, 1)
    place = down - across - INNER
    inside = jnp.logical_and(place >= 0, place < REACH)
    low_lane = across < HALF
    place_far = lax.rem(down - across - INNER - HALF + 4 * LANES, 2 * LANES)
    inside_outer = jnp.where(low_lane, jnp.where(inside, 1, 0), jnp.where(place_far < REACH, 1, 0)) > 0
    for k in range(NK):
        row_mats[k] = skewed(row_table[k : k + 1], UNIT).astype(BF16)
        near = skewed(backward[k : k + 1], 2 * LANES)
        far = skewed(backward_half[k : k + 1], 2 * LANES)
        half = slice((k % 2) * LANES, (k % 2 + 1) * LANES)
        column_mats[k // 2, :, half] = jnp.where(inside, near, 0.0).astype(BF16)
        outer_mats[k // 2, :, half] = jnp.where(
            inside_outer, jnp.where(low_lane, near, far), 0.0
        ).astype(BF16)

    table = interp_ref[...].astype(F32)
    phases = lax.broadcasted_iota(jnp.int32, table.shape, 1)
    lane_wide = lax.broadcasted_iota(jnp.int32, (1, 2 * LANES), 1)
    lane_one = lax.broadcasted_iota(jnp.int32, (1, LANES), 1)

    def chosen(phase):
        row = jnp.sum(jnp.where(phases == phase, table, 0.0), axis=1, keepdims=True)
        return [row[t : t + 1] for t in range(2 * IH)]

    for b in range(count):
        u = chosen(phase_ref[0, 0, b])
        v = chosen(phase_ref[1, 0, b])
        lead = EDGE + 1 - IH + shift_ref[0, 0, b]
        row = jnp.zeros((1, 2 * LANES), F32)
        for tap in range(2 * IH):
            row = jnp.where(lane_wide == lead + tap, u[tap], row)
        warp_rows[b] = skewed(row, BLK).astype(BF16)
        lead = P_SIZE + 1 - IH + shift_ref[1, 0, b]
        row = jnp.zeros((1, LANES), F32)
        for tap in range(2 * IH):
            row = jnp.where(lane_one == LANES - lead - tap, v[tap], row)
        steep = skewed(row, 2 * LANES)
        spot = down - across - lead
        matrix = jnp.where(jnp.logical_and(spot >= 0, spot < 2 * IH), steep, 0.0)
        warp_columns[b] = matrix.astype(BF16)
        warp_last[b, :LANES, :] = matrix[:LANES].astype(BF16)
        warp_last[b, LANES : LANES + HALF, :] = jnp.zeros((HALF, LANES), BF16)
        warp_last[b, LANES + HALF :, :] = matrix[LANES : LANES + HALF].astype(BF16)

    def relay(peer, side):
        span = pl.ds(KH, height)
        source = recv.at[span, pl.ds(0 if side == 0 else strip - LANES, LANES)]
        target = after.at[span, :] if side == 0 else before.at[span, :]
        return pltpu.make_async_remote_copy(
            src_ref=source,
            dst_ref=target,
            send_sem=relay_send.at[side],
            recv_sem=relay_recv.at[side],
            device_id={"band": peer},
            device_id_type=pl.DeviceIdType.MESH,
        )

    to_left = jnp.logical_and(me > 0, me != n // 2)
    to_right = jnp.logical_and(me < n - 1, me != n // 2 - 1)
    middle = jnp.logical_or(me == n // 2, me == n // 2 - 1)

    def pass_on():
        @pl.when(to_left)
        def _():
            relay(me - 1, 0).start()

        @pl.when(to_right)
        def _():
            relay(me + 1, 1).start()

    def take_ends():
        @pl.when(to_right)
        def _():
            relay(me + 1, 0).wait_recv()

        @pl.when(to_left)
        def _():
            relay(me - 1, 1).wait_recv()

        @pl.when(middle)
        def _():
            settle(end_recv, height - rows, LANES)
            settle(end_load, rows, LANES)

    def finish_relays():
        @pl.when(to_left)
        def _():
            relay(me - 1, 0).wait_send()

        @pl.when(to_right)
        def _():
            relay(me + 1, 1).wait_send()

        @pl.when(me != n // 2)
        def _():
            settle(end_send.at[1], rows, LANES)

        @pl.when(me != n // 2 - 1)
        def _():
            settle(end_send.at[0], rows, LANES)

    def across_kernels(panels, mats):
        if mats is outer_mats:
            windows = [ends[...]]
        else:
            windows = []
            for p in panels:
                if p == 0:
                    piece = recv[:, :LANES]
                    windows.append(jnp.concatenate([piece, piece], axis=1))
                else:
                    windows.append(recv[:, (p - 1) * LANES : (p + 1) * LANES])
        stacked = jnp.concatenate(windows, axis=0) if len(windows) > 1 else windows[0]
        for pair in range(NK // 2):
            result = jnp.dot(stacked, mats[pair], preferred_element_type=F32).astype(BF16)
            for i, p in enumerate(panels):
                for j in range(2):
                    crossed[2 * pair + j, :, p * LANES : (p + 1) * LANES] = result[
                        i * tall : (i + 1) * tall, j * LANES : (j + 1) * LANES
                    ]

    def gather_ends():
        lane = lax.broadcasted_iota(jnp.int32, (tall, LANES), 1) < HALF
        ends[:, :LANES] = jnp.where(lane, after[...], before[...])
        ends[:, LANES:] = jnp.where(lane, recv[:, :LANES], recv[:, strip - LANES :])

    def render(panels):
        for g in range(0, len(panels), 2):
            group = panels[g : g + 2]
            start = 0
            for extent in split(height):
                total = jnp.zeros((extent, len(group) * LANES), F32)
                for k in range(NK):
                    window = slice(start, start + extent + 2 * KH)
                    pieces = [crossed[k, window, p * LANES : (p + 1) * LANES] for p in group]
                    field = jnp.dot(
                        row_mats[k, :extent, : extent + 2 * KH],
                        jnp.concatenate(pieces, axis=1) if len(pieces) > 1 else pieces[0],
                        preferred_element_type=F32,
                    )
                    total = total + weight_ref[k] * field * field
                into = slice(EDGE + start, EDGE + start + extent)
                for i, p in enumerate(group):
                    part = total[:, i * LANES : (i + 1) * LANES]
                    if p == tiles:
                        lanes = lax.broadcasted_iota(jnp.int32, (extent, LANES), 1)
                        column = me * strip + lanes - P_SIZE + jnp.where(
                            lanes < HALF, 0, strip - HALF
                        )
                        part = jnp.where(
                            jnp.logical_and(column >= 0, column < width), part, 0.0
                        ).astype(BF16)
                        intensity[into, strip:] = part
                        intensity[into, :LANES] = jnp.where(
                            lanes < LEAD, part, intensity[into, :LANES]
                        )
                    else:
                        intensity[into, p * LANES : (p + 1) * LANES] = part.astype(BF16)
                start += extent

    def halfway(panels):
        runs = []
        for p in sorted(panels):
            if runs and runs[-1][1] == p:
                runs[-1][1] = p + 1
            else:
                runs.append([p, p + 1])
        for b in range(count):
            for lo, hi in runs:
                partial[b * BLK : (b + 1) * BLK, lo * LANES : hi * LANES] = jnp.dot(
                    warp_rows[b, :, : BLK + 2 * EDGE],
                    intensity[b * BLK : (b + 1) * BLK + 2 * EDGE, lo * LANES : hi * LANES],
                    preferred_element_type=F32,
                ).astype(BF16)

    def finish(targets):
        targets = sorted(targets)
        common = [q for q in targets if q < tiles - 1]
        for b in range(count):
            own = slice(b * BLK, (b + 1) * BLK)
            care = care_ref[0, b].astype(F32)
            results = []
            if common:
                warped = jnp.dot(
                    jnp.concatenate(
                        [partial[own, q * LANES : (q + 2) * LANES] for q in common], axis=0
                    ),
                    warp_columns[b],
                    preferred_element_type=F32,
                )
                results += [(q, warped[i * BLK : (i + 1) * BLK]) for i, q in enumerate(common)]
            if tiles - 1 in targets:
                q = tiles - 1
                results.append(
                    (
                        q,
                        jnp.dot(
                            partial[own, q * LANES : (q + 2) * LANES], warp_last[b],
                            preferred_element_type=F32,
                        ),
                    )
                )
            for q, warped in results:
                measured = image[own, q * LANES : (q + 1) * LANES].astype(F32)
                diff[8 + b * BLK : 8 + (b + 1) * BLK, q * LANES : (q + 1) * LANES] = care * (
                    measured - warped
                )
        first = partial_sums[:8, :]
        second = partial_sums[8:, :]
        for q in targets:
            column = slice(q * LANES, (q + 1) * LANES)
            for start in range(0, height, BLK):
                around = diff[start : start + BLK + 16, column]
                value = around[8 : 8 + BLK] + 0.5 * (around[7 : 7 + BLK] + around[9 : 9 + BLK])
                filt[start : start + BLK, column] = value
                power = value * value
                for r in range(0, BLK, 8):
                    first = first + value[r : r + 8]
                    second = second + power[r : r + 8]
        partial_sums[:8, :] = first
        partial_sums[8:, :] = second

    loads[-1].wait()
    loads[-2].wait()
    seen, crossing, waiting, halves, done = set(), set(), [], set(), set()
    for e, event in enumerate(events):
        settle(recv_sem.at[e], *sizes[e])
        if e == 0:
            pass_on()
        send_after(e)
        for lo, span in event:
            seen.update(range(lo, lo + span))
        fresh = [
            p for p in range(tiles)
            if p in seen and (p == 0 or p - 1 in seen) and p not in crossing
        ]
        if fresh:
            across_kernels(fresh, column_mats)
        crossing.update(fresh)
        waiting += fresh
        if e == min(1, len(events) - 1):
            take_ends()
            gather_ends()
            across_kernels([tiles], outer_mats)
            waiting.append(tiles)
        if e == 0 and len(events) > 1:
            continue
        render(waiting)
        halfway(waiting)
        halves.update(waiting)
        waiting = []
        targets = {q for q in range(tiles) if q in halves and q + 1 in halves} - done
        finish(targets)
        done.update(targets)

    stats_mine[0:1, :] = jnp.sum(partial_sums[:8, :], axis=0, keepdims=True)
    stats_mine[1:2, :] = jnp.sum(partial_sums[8:, :], axis=0, keepdims=True)

    def stat_to(peer):
        return pltpu.make_async_remote_copy(
            src_ref=stats_mine,
            dst_ref=stats_all.at[me],
            send_sem=stat_send,
            recv_sem=stat_recv,
            device_id={"band": peer},
            device_id_type=pl.DeviceIdType.MESH,
        )

    for i in range(n - 1, 0, -1):
        stat_to(partner(i)).start()
    stats_all[me] = stats_mine[...]

    for slot, size in enumerate(sizes):
        settle(send_sem.at[slot], *size)
    finish_relays()

    others = stats_all.at[pl.ds(0, n - 1)]
    pltpu.make_async_copy(others, others, stat_send).wait()
    pltpu.make_async_copy(others, others, stat_recv).wait()
    sums = jnp.sum(stats_all[...], axis=0)
    cells = height * width
    totals = jnp.sum(sums, axis=1, keepdims=True) / cells
    mean, power = totals[0:1], totals[1:2]
    scale = lax.rsqrt(power - mean * mean + epsilon)
    mean_ref[...] = jnp.broadcast_to(mean, (1, strip))
    for b in range(count):
        scale_ref[b : b + 1, :] = jnp.broadcast_to(care_ref[0, b].astype(F32) * scale, (1, strip))


def on_device(
    design, row_taps, column_taps, kernel_weight, interp, block_shift, block_phase, care, image
):
    n = lax.axis_size("band")
    rows, width = design.shape
    height, strip = image.shape
    wide = strip + LANES
    count = height // BLK
    slots = len(plan(strip // LANES))
    tall = height + 2 * KH
    hbm = pl.BlockSpec(memory_space=pltpu.HBM)
    vmem = pl.BlockSpec(memory_space=pltpu.VMEM)
    filtered, mean, scale = pl.pallas_call(
        functools.partial(kernel, n, height, width),
        out_shape=(
            jax.ShapeDtypeStruct((height, strip), F32),
            jax.ShapeDtypeStruct((1, strip), F32),
            jax.ShapeDtypeStruct((count, strip), F32),
        ),
        in_specs=[hbm] * 9,
        out_specs=(vmem, vmem, vmem),
        scratch_shapes=[
            pltpu.SMEM((NK,), F32),
            pltpu.SMEM((2, 1, count), jnp.int32),
            pltpu.SMEM((2, 1, count), jnp.int32),
            pltpu.SMEM((1, count), jnp.int32),
            pltpu.VMEM(row_taps.shape, BF16),
            pltpu.VMEM(column_taps.shape, BF16),
            pltpu.VMEM(interp.shape[::-1], BF16),
            pltpu.VMEM((tall, strip), BF16),
            pltpu.VMEM((tall, LANES), BF16),
            pltpu.VMEM((tall, LANES), BF16),
            pltpu.VMEM((tall, 2 * LANES), BF16),
            pltpu.VMEM((height, strip), BF16),
            pltpu.VMEM((NK, UNIT, 2 * LANES), BF16),
            pltpu.VMEM((NK // 2, 2 * LANES, 2 * LANES), BF16),
            pltpu.VMEM((NK // 2, 2 * LANES, 2 * LANES), BF16),
            pltpu.VMEM((count, BLK, 2 * LANES), BF16),
            pltpu.VMEM((count, 2 * LANES, LANES), BF16),
            pltpu.VMEM((count, 2 * LANES, LANES), BF16),
            pltpu.VMEM((NK, tall, wide), BF16),
            pltpu.VMEM((height + 2 * EDGE, wide), BF16),
            pltpu.VMEM((height, wide), BF16),
            pltpu.VMEM((height + 16, strip), F32),
            pltpu.VMEM((16, LANES), F32),
            pltpu.VMEM((2, LANES), F32),
            pltpu.VMEM((n, 2, LANES), F32),
            pltpu.SemaphoreType.DMA((slots,)),
            pltpu.SemaphoreType.DMA((slots,)),
            pltpu.SemaphoreType.DMA((2,)),
            pltpu.SemaphoreType.DMA((2,)),
            pltpu.SemaphoreType.DMA((2,)),
            pltpu.SemaphoreType.DMA,
            pltpu.SemaphoreType.DMA,
            pltpu.SemaphoreType.DMA,
            pltpu.SemaphoreType.DMA,
            pltpu.SemaphoreType.DMA((9,)),
        ],
        compiler_params=pltpu.CompilerParams(
            collective_id=0, has_side_effects=True, vmem_limit_bytes=48 * 1024 * 1024
        ),
    )(
        pin(kernel_weight),
        pin(jnp.transpose(block_shift, (0, 2, 1))),
        pin(jnp.transpose(block_phase, (0, 2, 1))),
        pin(care.T),
        pin(design),
        pin(row_taps),
        pin(column_taps),
        pin(interp.T),
        pin(image),
    )
    blocks = filtered.reshape(count, BLK, strip)
    out = (blocks - mean[:, None]) * scale[:, None]
    return out.reshape(height, strip).astype(BF16)


def solution(mesh):
    placed = (
        P(("swath", "band"), None),
        P(),
        P(),
        P(),
        P(),
        P(None, "swath", "band"),
        P(None, "swath", "band"),
        P("swath", "band"),
        P("swath", "band"),
    )
    return jax.shard_map(
        on_device, mesh=mesh, in_specs=placed, out_specs=P("swath", "band"), check_vma=False
    )
```

```python
import functools

import jax
import jax.numpy as jnp
from jax import lax
from jax.experimental import pallas as pl
from jax.experimental.pallas import tpu as pltpu
from jax.sharding import PartitionSpec as P

NK = 8
KH = 16
IH = 4
BLK = 128
P_SIZE = 28
LANES = 128
HALF = LANES // 2
EDGE = 32
UNIT = 128
REACH = 2 * KH + 1
LEAD = P_SIZE + KH
INNER = LANES - LEAD

LEVELS = 4
LATE = (3,)

epsilon = 1e-05

F32 = jnp.float32
BF16 = jnp.bfloat16


def pin(x):
    return pltpu.with_memory_space_constraint(x, pltpu.HBM)


def skewed(row, rows):
    base = jnp.broadcast_to(row, (rows, row.shape[1]))
    return pltpu.roll(base, 0, 1, stride=1, stride_axis=0)


def split(total):
    return [min(UNIT, total - at) for at in range(0, total, UNIT)]


def plan(tiles):
    if tiles < 4:
        return [[(0, tiles)]]
    events = [[(0, 1), (tiles - 1, 1)]]
    low, high = 1, tiles - 2
    left = True
    while low <= high:
        span = min(2, high - low + 1)
        events.append([(low if left else high - span + 1, span)])
        low, high = (low + span, high) if left else (low, high - span)
        left = not left
    return events


def kernel(
    n, height, width,
    weight_hbm, shift_hbm, phase_hbm, care_hbm,
    design_hbm, row_hbm, column_hbm, interp_hbm, image_hbm,
    filt, mean_ref, scale_ref,
    weight_ref, shift_ref, phase_ref, care_ref,
    row_ref, column_ref, interp_ref,
    recv, before, after, ends, image, row_mats, column_mats, outer_mats,
    warp_rows, warp_columns, warp_last, crossed, intensity, partial,
    diff, partial_sums, stats_mine, stats_all,
    send_sem, recv_sem, relay_send, relay_recv, end_send, end_recv, end_load, stat_send, stat_recv, two_away, three_away, load_sem,
):
    me = lax.axis_index("band")
    rows = height // n
    strip = width // n
    tiles = strip // LANES
    tall = height + 2 * KH
    count = height // BLK
    events = plan(tiles)

    barrier = pltpu.get_barrier_semaphore()

    mine = pl.ds(pl.multiple_of(KH + me * rows, rows), rows)
    loads = [
        pltpu.make_async_copy(source, target, load_sem.at[i])
        for i, (source, target) in enumerate(
            [
                (row_hbm, row_ref),
                (column_hbm, column_ref),
                (interp_hbm, interp_ref),
                (weight_hbm, weight_ref),
                (shift_hbm, shift_ref),
                (phase_hbm, phase_ref),
                (care_hbm, care_ref),
                (image_hbm, image),
                (
                    design_hbm.at[:, pl.ds(pl.multiple_of(me * strip, LANES), strip)],
                    recv.at[mine, :],
                ),
            ]
        )
    ]
    flips = {}
    bit = 1
    while bit < n:
        flips[bit] = bit * (1 - 2 * lax.rem(me // bit, 2))
        bit *= 2

    def partner(i):
        return me + sum(flip for bit, flip in flips.items() if i & bit)

    def send(peer, slot, lo, span):
        pltpu.make_async_remote_copy(
            src_ref=design_hbm.at[
                :, pl.ds(pl.multiple_of(peer * strip + lo * LANES, LANES), span * LANES)
            ],
            dst_ref=recv.at[mine, pl.ds(lo * LANES, span * LANES)],
            send_sem=send_sem.at[slot],
            recv_sem=recv_sem.at[slot],
            device_id={"band": peer},
            device_id_type=pl.DeviceIdType.MESH,
        ).start()

    def send_ends():
        for target, edge, tile in ((n // 2, before, -1), (n // 2 - 1, after, 0)):
            source = design_hbm.at[:, pl.ds((n // 2) * strip + tile * LANES, LANES)]
            place = edge.at[mine, :]

            @pl.when(me != target)
            def _():
                pltpu.make_async_remote_copy(
                    src_ref=source,
                    dst_ref=place,
                    send_sem=end_send.at[-tile],
                    recv_sem=end_recv,
                    device_id={"band": jnp.int32(target)},
                    device_id_type=pl.DeviceIdType.MESH,
                ).start()

            @pl.when(me == target)
            def _():
                pltpu.make_async_copy(source, place, end_load).start()

    def block(extent, columns):
        return recv.at[pl.ds(0, extent), pl.ds(0, columns)]

    def settle(sem, extent, columns):
        pltpu.make_async_copy(block(extent, columns), block(extent, columns), sem).wait()

    sizes = [(height - rows, sum(span for _, span in event) * LANES) for event in events]

    level = me // (n // LEVELS)
    inner = jnp.logical_and(level > 0, level < LEVELS - 1)
    outer = jnp.logical_not(inner)
    near = range(1, n // 2)
    second = range(n // 2, 3 * n // 4)
    third = range(3 * n // 4, n)

    def send_to(e, ids):
        for i in ids:
            for lo, span in events[e]:
                send(partner(i), e, lo, span)

    def tell(semaphore, i):
        pl.semaphore_signal(
            semaphore, inc=1, device_id={"band": partner(i)}, device_id_type=pl.DeviceIdType.MESH
        )

    for i in near:
        tell(barrier, i)

    @pl.when(inner)
    def _():
        for i in third:
            tell(barrier, i)

    for load in loads:
        load.start()
    pl.semaphore_wait(barrier, n // 2 - 1 + jnp.where(inner, n // 4, 0))
    early = range(1, min(2, len(events)))

    @pl.when(inner)
    def _():
        tell(two_away, n // LEVELS)
        tell(two_away, 3 * n // LEVELS)

    send_to(0, near)

    @pl.when(inner)
    def _():
        send_to(0, third)

        @pl.when(level == 1)
        def _():
            for e in early:
                send_to(e, third)

        pl.semaphore_wait(two_away, 1)
        tell(three_away, n // LEVELS)
        send_to(0, second)

    @pl.when(outer)
    def _():
        pl.semaphore_wait(two_away, 1)
        send_to(0, second)
        pl.semaphore_wait(three_away, 1)
        send_to(0, third)

    send_ends()
    for e in early:
        send_to(e, near)
        send_to(e, second)

        @pl.when(jnp.logical_not(level == 1))
        def _():
            send_to(e, third)

    def send_rest(late):
        for e in range(2, len(events)):
            if (e in LATE) == late:
                send_to(e, range(1, n))

    send_rest(False)

    for k in range(NK):
        crossed[k, :KH, :] = jnp.zeros((KH, strip + LANES), BF16)
        crossed[k, KH + height :, :] = jnp.zeros((KH, strip + LANES), BF16)

    @pl.when(me == 0)
    def _():
        before[KH : KH + height, :] = jnp.zeros((height, LANES), BF16)

    @pl.when(me == n - 1)
    def _():
        after[KH : KH + height, :] = jnp.zeros((height, LANES), BF16)

    wide = strip + LANES
    intensity[:EDGE, :] = jnp.zeros((EDGE, wide), BF16)
    intensity[EDGE + height :, :] = jnp.zeros((EDGE, wide), BF16)
    diff[:8, :] = jnp.zeros((8, strip), F32)
    diff[8 + height :, :] = jnp.zeros((8, strip), F32)
    partial_sums[...] = jnp.zeros((16, LANES), F32)

    for load in loads[:-2]:
        load.wait()

    pad = jnp.zeros((NK, LANES - REACH), F32)
    row_table = jnp.concatenate([row_ref[...].astype(F32), pad, jnp.zeros((NK, LANES), F32)], axis=1)
    column_table = jnp.concatenate([column_ref[...].astype(F32), pad], axis=1)
    from_lane = lax.broadcasted_iota(jnp.int32, (LANES, LANES), 0)
    to_lane = lax.broadcasted_iota(jnp.int32, (LANES, LANES), 1)
    turned = jnp.where(lax.rem(2 * LANES - INNER - to_lane, LANES) == from_lane, 1.0, 0.0)
    backward = jnp.dot(
        column_table.astype(BF16), turned.astype(BF16), preferred_element_type=F32
    )
    backward_half = pltpu.roll(backward, HALF, 1)
    square = (2 * LANES, LANES)
    down = lax.broadcasted_iota(jnp.int32, square, 0)
    across = lax.broadcasted_iota(jnp.int32, square, 1)
    place = down - across - INNER
    inside = jnp.logical_and(place >= 0, place < REACH)
    low_lane = across < HALF
    place_far = lax.rem(down - across - INNER - HALF + 4 * LANES, 2 * LANES)
    inside_outer = jnp.where(low_lane, jnp.where(inside, 1, 0), jnp.where(place_far < REACH, 1, 0)) > 0
    for k in range(NK):
        row_mats[k] = skewed(row_table[k : k + 1], UNIT).astype(BF16)
        near = skewed(backward[k : k + 1], 2 * LANES)
        far = skewed(backward_half[k : k + 1], 2 * LANES)
        half = slice((k % 2) * LANES, (k % 2 + 1) * LANES)
        column_mats[k // 2, :, half] = jnp.where(inside, near, 0.0).astype(BF16)
        outer_mats[k // 2, :, half] = jnp.where(
            inside_outer, jnp.where(low_lane, near, far), 0.0
        ).astype(BF16)

    table = interp_ref[...].astype(F32)
    phases = lax.broadcasted_iota(jnp.int32, table.shape, 1)
    lane_wide = lax.broadcasted_iota(jnp.int32, (1, 2 * LANES), 1)
    lane_one = lax.broadcasted_iota(jnp.int32, (1, LANES), 1)

    def chosen(phase):
        row = jnp.sum(jnp.where(phases == phase, table, 0.0), axis=1, keepdims=True)
        return [row[t : t + 1] for t in range(2 * IH)]

    for b in range(count):
        u = chosen(phase_ref[0, 0, b])
        v = chosen(phase_ref[1, 0, b])
        lead = EDGE + 1 - IH + shift_ref[0, 0, b]
        row = jnp.zeros((1, 2 * LANES), F32)
        for tap in range(2 * IH):
            row = jnp.where(lane_wide == lead + tap, u[tap], row)
        warp_rows[b] = skewed(row, BLK).astype(BF16)
        lead = P_SIZE + 1 - IH + shift_ref[1, 0, b]
        row = jnp.zeros((1, LANES), F32)
        for tap in range(2 * IH):
            row = jnp.where(lane_one == LANES - lead - tap, v[tap], row)
        steep = skewed(row, 2 * LANES)
        spot = down - across - lead
        matrix = jnp.where(jnp.logical_and(spot >= 0, spot < 2 * IH), steep, 0.0)
        warp_columns[b] = matrix.astype(BF16)
        warp_last[b, :LANES, :] = matrix[:LANES].astype(BF16)
        warp_last[b, LANES : LANES + HALF, :] = jnp.zeros((HALF, LANES), BF16)
        warp_last[b, LANES + HALF :, :] = matrix[LANES : LANES + HALF].astype(BF16)

    def relay(peer, side):
        span = pl.ds(KH, height)
        source = recv.at[span, pl.ds(0 if side == 0 else strip - LANES, LANES)]
        target = after.at[span, :] if side == 0 else before.at[span, :]
        return pltpu.make_async_remote_copy(
            src_ref=source,
            dst_ref=target,
            send_sem=relay_send.at[side],
            recv_sem=relay_recv.at[side],
            device_id={"band": peer},
            device_id_type=pl.DeviceIdType.MESH,
        )

    to_left = jnp.logical_and(me > 0, me != n // 2)
    to_right = jnp.logical_and(me < n - 1, me != n // 2 - 1)
    middle = jnp.logical_or(me == n // 2, me == n // 2 - 1)

    def pass_on():
        @pl.when(to_left)
        def _():
            relay(me - 1, 0).start()

        @pl.when(to_right)
        def _():
            relay(me + 1, 1).start()

    def take_ends():
        @pl.when(to_right)
        def _():
            relay(me + 1, 0).wait_recv()

        @pl.when(to_left)
        def _():
            relay(me - 1, 1).wait_recv()

        @pl.when(middle)
        def _():
            settle(end_recv, height - rows, LANES)
            settle(end_load, rows, LANES)

    def finish_relays():
        @pl.when(to_left)
        def _():
            relay(me - 1, 0).wait_send()

        @pl.when(to_right)
        def _():
            relay(me + 1, 1).wait_send()

        @pl.when(me != n // 2)
        def _():
            settle(end_send.at[1], rows, LANES)

        @pl.when(me != n // 2 - 1)
        def _():
            settle(end_send.at[0], rows, LANES)

    body = slice(KH, KH + height)

    def across_kernels(panels, mats):
        if mats is outer_mats:
            windows = [ends[...]]
        else:
            windows = []
            for p in panels:
                if p == 0:
                    piece = recv[body, :LANES]
                    windows.append(jnp.concatenate([piece, piece], axis=1))
                else:
                    windows.append(recv[body, (p - 1) * LANES : (p + 1) * LANES])
        stacked = jnp.concatenate(windows, axis=0) if len(windows) > 1 else windows[0]
        for pair in range(NK // 2):
            result = jnp.dot(stacked, mats[pair], preferred_element_type=F32).astype(BF16)
            for i, p in enumerate(panels):
                for j in range(2):
                    crossed[2 * pair + j, body, p * LANES : (p + 1) * LANES] = result[
                        i * height : (i + 1) * height, j * LANES : (j + 1) * LANES
                    ]

    def gather_ends():
        lane = lax.broadcasted_iota(jnp.int32, (height, LANES), 1) < HALF
        ends[:, :LANES] = jnp.where(lane, after[body, :], before[body, :])
        ends[:, LANES:] = jnp.where(lane, recv[body, :LANES], recv[body, strip - LANES :])

    def render(panels):
        for g in range(0, len(panels), 2):
            group = panels[g : g + 2]
            start = 0
            for extent in split(height):
                total = jnp.zeros((extent, len(group) * LANES), F32)
                for k in range(NK):
                    window = slice(start, start + extent + 2 * KH)
                    pieces = [crossed[k, window, p * LANES : (p + 1) * LANES] for p in group]
                    field = jnp.dot(
                        row_mats[k, :extent, : extent + 2 * KH],
                        jnp.concatenate(pieces, axis=1) if len(pieces) > 1 else pieces[0],
                        preferred_element_type=F32,
                    )
                    total = total + weight_ref[k] * field * field
                into = slice(EDGE + start, EDGE + start + extent)
                for i, p in enumerate(group):
                    part = total[:, i * LANES : (i + 1) * LANES]
                    if p == tiles:
                        lanes = lax.broadcasted_iota(jnp.int32, (extent, LANES), 1)
                        column = me * strip + lanes - P_SIZE + jnp.where(
                            lanes < HALF, 0, strip - HALF
                        )
                        part = jnp.where(
                            jnp.logical_and(column >= 0, column < width), part, 0.0
                        ).astype(BF16)
                        intensity[into, strip:] = part
                        intensity[into, :LANES] = jnp.where(
                            lanes < LEAD, part, intensity[into, :LANES]
                        )
                    else:
                        intensity[into, p * LANES : (p + 1) * LANES] = part.astype(BF16)
                start += extent

    def halfway(panels):
        runs = []
        for p in sorted(panels):
            if runs and runs[-1][1] == p:
                runs[-1][1] = p + 1
            else:
                runs.append([p, p + 1])
        for b in range(count):
            for lo, hi in runs:
                partial[b * BLK : (b + 1) * BLK, lo * LANES : hi * LANES] = jnp.dot(
                    warp_rows[b, :, : BLK + 2 * EDGE],
                    intensity[b * BLK : (b + 1) * BLK + 2 * EDGE, lo * LANES : hi * LANES],
                    preferred_element_type=F32,
                ).astype(BF16)

    def finish(targets):
        targets = sorted(targets)
        common = [q for q in targets if q < tiles - 1]
        for b in range(count):
            own = slice(b * BLK, (b + 1) * BLK)
            care = care_ref[0, b].astype(F32)
            results = []
            if common:
                warped = jnp.dot(
                    jnp.concatenate(
                        [partial[own, q * LANES : (q + 2) * LANES] for q in common], axis=0
                    ),
                    warp_columns[b],
                    preferred_element_type=F32,
                )
                results += [(q, warped[i * BLK : (i + 1) * BLK]) for i, q in enumerate(common)]
            if tiles - 1 in targets:
                q = tiles - 1
                results.append(
                    (
                        q,
                        jnp.dot(
                            partial[own, q * LANES : (q + 2) * LANES], warp_last[b],
                            preferred_element_type=F32,
                        ),
                    )
                )
            for q, warped in results:
                measured = image[own, q * LANES : (q + 1) * LANES].astype(F32)
                diff[8 + b * BLK : 8 + (b + 1) * BLK, q * LANES : (q + 1) * LANES] = care * (
                    measured - warped
                )
        first = partial_sums[:8, :]
        second = partial_sums[8:, :]
        for q in targets:
            column = slice(q * LANES, (q + 1) * LANES)
            for start in range(0, height, BLK):
                around = diff[start : start + BLK + 16, column]
                value = around[8 : 8 + BLK] + 0.5 * (around[7 : 7 + BLK] + around[9 : 9 + BLK])
                filt[start : start + BLK, column] = value
                power = value * value
                for r in range(0, BLK, 8):
                    first = first + value[r : r + 8]
                    second = second + power[r : r + 8]
        partial_sums[:8, :] = first
        partial_sums[8:, :] = second

    loads[-1].wait()
    loads[-2].wait()
    seen, crossing, waiting, halves, done = set(), set(), [], set(), set()
    halves_due = []
    for e, event in enumerate(events):
        settle(recv_sem.at[e], *sizes[e])
        if e == 0:
            pass_on()
        if e == 0:
            send_rest(True)
        for lo, span in event:
            seen.update(range(lo, lo + span))
        fresh = [
            p for p in range(tiles)
            if p in seen and (p == 0 or p - 1 in seen) and p not in crossing
        ]
        if fresh:
            across_kernels(fresh, column_mats)
        crossing.update(fresh)
        waiting += fresh
        if e == min(1, len(events) - 1):
            take_ends()
            gather_ends()
            across_kernels([tiles], outer_mats)
            waiting.append(tiles)
        render(waiting)
        if e == 0 and len(events) > 1:
            halves_due = waiting
            waiting = []
            continue
        waiting = halves_due + waiting
        halves_due = []
        halfway(waiting)
        halves.update(waiting)
        waiting = []
        targets = {q for q in range(tiles) if q in halves and q + 1 in halves} - done
        finish(targets)
        done.update(targets)

    stats_mine[0:1, :] = jnp.sum(partial_sums[:8, :], axis=0, keepdims=True)
    stats_mine[1:2, :] = jnp.sum(partial_sums[8:, :], axis=0, keepdims=True)

    def stat_to(peer):
        return pltpu.make_async_remote_copy(
            src_ref=stats_mine,
            dst_ref=stats_all.at[me],
            send_sem=stat_send,
            recv_sem=stat_recv,
            device_id={"band": peer},
            device_id_type=pl.DeviceIdType.MESH,
        )

    for i in range(n - 1, 0, -1):
        stat_to(partner(i)).start()
    stats_all[me] = stats_mine[...]

    for slot, size in enumerate(sizes):
        settle(send_sem.at[slot], *size)
    finish_relays()

    others = stats_all.at[pl.ds(0, n - 1)]
    pltpu.make_async_copy(others, others, stat_send).wait()
    pltpu.make_async_copy(others, others, stat_recv).wait()
    sums = jnp.sum(stats_all[...], axis=0)
    cells = height * width
    totals = jnp.sum(sums, axis=1, keepdims=True) / cells
    mean, power = totals[0:1], totals[1:2]
    scale = lax.rsqrt(power - mean * mean + epsilon)
    mean_ref[...] = jnp.broadcast_to(mean, (1, strip))
    for b in range(count):
        scale_ref[b : b + 1, :] = jnp.broadcast_to(care_ref[0, b].astype(F32) * scale, (1, strip))


def on_device(
    design, row_taps, column_taps, kernel_weight, interp, block_shift, block_phase, care, image
):
    n = lax.axis_size("band")
    rows, width = design.shape
    height, strip = image.shape
    wide = strip + LANES
    count = height // BLK
    slots = len(plan(strip // LANES))
    tall = height + 2 * KH
    hbm = pl.BlockSpec(memory_space=pltpu.HBM)
    vmem = pl.BlockSpec(memory_space=pltpu.VMEM)
    filtered, mean, scale = pl.pallas_call(
        functools.partial(kernel, n, height, width),
        out_shape=(
            jax.ShapeDtypeStruct((height, strip), F32),
            jax.ShapeDtypeStruct((1, strip), F32),
            jax.ShapeDtypeStruct((count, strip), F32),
        ),
        in_specs=[hbm] * 9,
        out_specs=(vmem, vmem, vmem),
        scratch_shapes=[
            pltpu.SMEM((NK,), F32),
            pltpu.SMEM((2, 1, count), jnp.int32),
            pltpu.SMEM((2, 1, count), jnp.int32),
            pltpu.SMEM((1, count), jnp.int32),
            pltpu.VMEM(row_taps.shape, BF16),
            pltpu.VMEM(column_taps.shape, BF16),
            pltpu.VMEM(interp.shape[::-1], BF16),
            pltpu.VMEM((tall, strip), BF16),
            pltpu.VMEM((tall, LANES), BF16),
            pltpu.VMEM((tall, LANES), BF16),
            pltpu.VMEM((height, 2 * LANES), BF16),
            pltpu.VMEM((height, strip), BF16),
            pltpu.VMEM((NK, UNIT, 2 * LANES), BF16),
            pltpu.VMEM((NK // 2, 2 * LANES, 2 * LANES), BF16),
            pltpu.VMEM((NK // 2, 2 * LANES, 2 * LANES), BF16),
            pltpu.VMEM((count, BLK, 2 * LANES), BF16),
            pltpu.VMEM((count, 2 * LANES, LANES), BF16),
            pltpu.VMEM((count, 2 * LANES, LANES), BF16),
            pltpu.VMEM((NK, tall, wide), BF16),
            pltpu.VMEM((height + 2 * EDGE, wide), BF16),
            pltpu.VMEM((height, wide), BF16),
            pltpu.VMEM((height + 16, strip), F32),
            pltpu.VMEM((16, LANES), F32),
            pltpu.VMEM((2, LANES), F32),
            pltpu.VMEM((n, 2, LANES), F32),
            pltpu.SemaphoreType.DMA((slots,)),
            pltpu.SemaphoreType.DMA((slots,)),
            pltpu.SemaphoreType.DMA((2,)),
            pltpu.SemaphoreType.DMA((2,)),
            pltpu.SemaphoreType.DMA((2,)),
            pltpu.SemaphoreType.DMA,
            pltpu.SemaphoreType.DMA,
            pltpu.SemaphoreType.DMA,
            pltpu.SemaphoreType.DMA,
            pltpu.SemaphoreType.REGULAR,
            pltpu.SemaphoreType.REGULAR,
            pltpu.SemaphoreType.DMA((9,)),
        ],
        compiler_params=pltpu.CompilerParams(
            collective_id=0, has_side_effects=True, vmem_limit_bytes=48 * 1024 * 1024
        ),
    )(
        pin(kernel_weight),
        pin(jnp.transpose(block_shift, (0, 2, 1))),
        pin(jnp.transpose(block_phase, (0, 2, 1))),
        pin(care.T),
        pin(design),
        pin(row_taps),
        pin(column_taps),
        pin(interp.T),
        pin(image),
    )
    blocks = filtered.reshape(count, BLK, strip)
    out = (blocks - mean[:, None]) * scale[:, None]
    return out.reshape(height, strip).astype(BF16)


def solution(mesh):
    placed = (
        P(("swath", "band"), None),
        P(),
        P(),
        P(),
        P(),
        P(None, "swath", "band"),
        P(None, "swath", "band"),
        P("swath", "band"),
        P("swath", "band"),
    )
    return jax.shard_map(
        on_device, mesh=mesh, in_specs=placed, out_specs=P("swath", "band"), check_vma=False
    )
```

```python
import functools

import jax
import jax.numpy as jnp
from jax import lax
from jax.experimental import pallas as pl
from jax.experimental.pallas import tpu as pltpu
from jax.sharding import PartitionSpec as P

NK = 8
KH = 16
IH = 4
BLK = 128
P_SIZE = 28
LANES = 128
HALF = LANES // 2
EDGE = 32
PIECE = 64
UNIT = 128
REACH = 2 * KH + 1
LEAD = P_SIZE + KH
INNER = LANES - LEAD

LEVELS = 4
LATE = (3,)

epsilon = 1e-05

F32 = jnp.float32
BF16 = jnp.bfloat16


def pin(x):
    return pltpu.with_memory_space_constraint(x, pltpu.HBM)


def skewed(row, rows):
    base = jnp.broadcast_to(row, (rows, row.shape[1]))
    return pltpu.roll(base, 0, 1, stride=1, stride_axis=0)


def split(total):
    return [min(UNIT, total - at) for at in range(0, total, UNIT)]


def plan(tiles):
    if tiles < 4:
        return [[(0, tiles)]]
    events = [[(0, 1), (tiles - 1, 1)]]
    low, high = 1, tiles - 2
    left = True
    while low <= high:
        span = min(2, high - low + 1)
        events.append([(low if left else high - span + 1, span)])
        low, high = (low + span, high) if left else (low, high - span)
        left = not left
    return events


def kernel(
    n, height, width,
    weight_hbm, shift_hbm, phase_hbm, care_hbm,
    design_hbm, row_hbm, column_hbm, interp_hbm, image_hbm,
    filt, mean_ref, scale_ref,
    weight_ref, shift_ref, phase_ref, care_ref,
    row_ref, column_ref, interp_ref,
    recv, before, after, ends, image, row_mats, column_mats, outer_mats,
    warp_rows, warp_columns, warp_last, crossed, intensity, partial,
    diff, partial_sums, stats_mine, stats_all,
    send_sem, recv_sem, relay_send, relay_recv, end_send, end_recv, end_load, stat_send, stat_recv, two_away, three_away, load_sem,
):
    me = lax.axis_index("band")
    rows = height // n
    strip = width // n
    tiles = strip // LANES
    tall = height + 2 * KH
    count = height // BLK
    events = plan(tiles)

    barrier = pltpu.get_barrier_semaphore()

    mine = pl.ds(pl.multiple_of(KH + me * rows, rows), rows)
    loads = [
        pltpu.make_async_copy(source, target, load_sem.at[i])
        for i, (source, target) in enumerate(
            [
                (row_hbm, row_ref),
                (column_hbm, column_ref),
                (interp_hbm, interp_ref),
                (weight_hbm, weight_ref),
                (shift_hbm, shift_ref),
                (phase_hbm, phase_ref),
                (care_hbm, care_ref),
                (image_hbm, image),
                (
                    design_hbm.at[:, pl.ds(pl.multiple_of(me * strip, LANES), strip)],
                    recv.at[mine, :],
                ),
            ]
        )
    ]
    flips = {}
    bit = 1
    while bit < n:
        flips[bit] = bit * (1 - 2 * lax.rem(me // bit, 2))
        bit *= 2

    def partner(i):
        return me + sum(flip for bit, flip in flips.items() if i & bit)

    def send(peer, slot, lo, span, far):
        pltpu.make_async_remote_copy(
            src_ref=design_hbm.at[
                :, pl.ds(pl.multiple_of(peer * strip + lo * LANES, LANES), span * LANES)
            ],
            dst_ref=recv.at[mine, pl.ds(lo * LANES, span * LANES)],
            send_sem=send_sem.at[slot, far],
            recv_sem=recv_sem.at[slot, far],
            device_id={"band": peer},
            device_id_type=pl.DeviceIdType.MESH,
        ).start()

    def send_ends():
        for target, edge, tile in ((n // 2, before, -1), (n // 2 - 1, after, 0)):
            source = design_hbm.at[:, pl.ds((n // 2) * strip + tile * LANES, LANES)]
            place = edge.at[mine, :]

            @pl.when(me != target)
            def _():
                pltpu.make_async_remote_copy(
                    src_ref=source,
                    dst_ref=place,
                    send_sem=end_send.at[-tile],
                    recv_sem=end_recv,
                    device_id={"band": jnp.int32(target)},
                    device_id_type=pl.DeviceIdType.MESH,
                ).start()

            @pl.when(me == target)
            def _():
                pltpu.make_async_copy(source, place, end_load).start()

    def block(extent, columns):
        return recv.at[pl.ds(0, extent), pl.ds(0, columns)]

    def settle(sem, extent, columns):
        pltpu.make_async_copy(block(extent, columns), block(extent, columns), sem).wait()

    half_rows = height // 2
    sizes = [sum(span for _, span in event) * LANES for event in events]

    level = me // (n // LEVELS)
    inner = jnp.logical_and(level > 0, level < LEVELS - 1)
    outer = jnp.logical_not(inner)
    near = range(1, n // 2)
    second = range(n // 2, 3 * n // 4)
    third = range(3 * n // 4, n)

    def send_to(e, ids):
        for i in ids:
            for lo, span in events[e]:
                send(partner(i), e, lo, span, int(i >= n // 2))

    def tell(semaphore, i):
        pl.semaphore_signal(
            semaphore, inc=1, device_id={"band": partner(i)}, device_id_type=pl.DeviceIdType.MESH
        )

    for i in near:
        tell(barrier, i)

    @pl.when(inner)
    def _():
        for i in third:
            tell(barrier, i)

    for load in loads:
        load.start()
    pl.semaphore_wait(barrier, n // 2 - 1 + jnp.where(inner, n // 4, 0))
    early = range(1, min(2, len(events)))

    @pl.when(inner)
    def _():
        tell(two_away, n // LEVELS)
        tell(two_away, 3 * n // LEVELS)

    send_to(0, near)

    @pl.when(inner)
    def _():
        send_to(0, third)

        @pl.when(level == 1)
        def _():
            for e in early:
                send_to(e, third)

        pl.semaphore_wait(two_away, 1)
        tell(three_away, n // LEVELS)
        send_to(0, second)

    @pl.when(outer)
    def _():
        pl.semaphore_wait(two_away, 1)
        send_to(0, second)
        pl.semaphore_wait(three_away, 1)
        send_to(0, third)

    send_ends()
    for e in early:
        send_to(e, near)
        send_to(e, second)

        @pl.when(jnp.logical_not(level == 1))
        def _():
            send_to(e, third)

    def send_rest(late):
        if not late:
            for e in range(2, len(events)):
                send_to(e, near)
        for e in range(2, len(events)):
            if (e in LATE) == late:
                if not late:
                    send_to(e, range(n // 2, n))
                    continue

                @pl.when(inner)
                def _():
                    send_to(e, second)
                    send_to(e, third)

                @pl.when(outer)
                def _():
                    send_to(e, third)
                    send_to(e, second)

    send_rest(False)

    for k in range(NK):
        crossed[k, :KH, :] = jnp.zeros((KH, strip + LANES), BF16)
        crossed[k, KH + height :, :] = jnp.zeros((KH, strip + LANES), BF16)

    @pl.when(me == 0)
    def _():
        before[KH : KH + height, :] = jnp.zeros((height, LANES), BF16)

    @pl.when(me == n - 1)
    def _():
        after[KH : KH + height, :] = jnp.zeros((height, LANES), BF16)

    wide = strip + LANES
    intensity[:EDGE, :] = jnp.zeros((EDGE, wide), BF16)
    intensity[EDGE + height :, :] = jnp.zeros((EDGE, wide), BF16)
    diff[:8, :] = jnp.zeros((8, strip), F32)
    diff[8 + height :, :] = jnp.zeros((8, strip), F32)
    partial_sums[...] = jnp.zeros((16, LANES), F32)

    for load in loads[:-2]:
        load.wait()

    pad = jnp.zeros((NK, LANES - REACH), F32)
    row_table = jnp.concatenate([row_ref[...].astype(F32), pad, jnp.zeros((NK, LANES), F32)], axis=1)
    column_table = jnp.concatenate([column_ref[...].astype(F32), pad], axis=1)
    from_lane = lax.broadcasted_iota(jnp.int32, (LANES, LANES), 0)
    to_lane = lax.broadcasted_iota(jnp.int32, (LANES, LANES), 1)
    turned = jnp.where(lax.rem(2 * LANES - INNER - to_lane, LANES) == from_lane, 1.0, 0.0)
    backward = jnp.dot(
        column_table.astype(BF16), turned.astype(BF16), preferred_element_type=F32
    )
    backward_half = pltpu.roll(backward, HALF, 1)
    square = (2 * LANES, LANES)
    down = lax.broadcasted_iota(jnp.int32, square, 0)
    across = lax.broadcasted_iota(jnp.int32, square, 1)
    place = down - across - INNER
    inside = jnp.logical_and(place >= 0, place < REACH)
    low_lane = across < HALF
    place_far = lax.rem(down - across - INNER - HALF + 4 * LANES, 2 * LANES)
    inside_outer = jnp.where(low_lane, jnp.where(inside, 1, 0), jnp.where(place_far < REACH, 1, 0)) > 0
    for k in range(NK):
        row_mats[k] = skewed(row_table[k : k + 1], UNIT).astype(BF16)
        near = skewed(backward[k : k + 1], 2 * LANES)
        far = skewed(backward_half[k : k + 1], 2 * LANES)
        half = slice((k % 2) * LANES, (k % 2 + 1) * LANES)
        column_mats[k // 2, :, half] = jnp.where(inside, near, 0.0).astype(BF16)
        outer_mats[k // 2, :, half] = jnp.where(
            inside_outer, jnp.where(low_lane, near, far), 0.0
        ).astype(BF16)

    table = interp_ref[...].astype(F32)
    phases = lax.broadcasted_iota(jnp.int32, table.shape, 1)
    lane_wide = lax.broadcasted_iota(jnp.int32, (1, 2 * LANES), 1)
    lane_one = lax.broadcasted_iota(jnp.int32, (1, LANES), 1)

    def chosen(phase):
        row = jnp.sum(jnp.where(phases == phase, table, 0.0), axis=1, keepdims=True)
        return [row[t : t + 1] for t in range(2 * IH)]

    for b in range(count):
        u = chosen(phase_ref[0, 0, b])
        v = chosen(phase_ref[1, 0, b])
        lead = EDGE + 1 - IH + shift_ref[0, 0, b]
        row = jnp.zeros((1, 2 * LANES), F32)
        for tap in range(2 * IH):
            row = jnp.where(lane_wide == lead + tap, u[tap], row)
        warp_rows[b] = skewed(row, BLK).astype(BF16)
        lead = P_SIZE + 1 - IH + shift_ref[1, 0, b]
        row = jnp.zeros((1, LANES), F32)
        for tap in range(2 * IH):
            row = jnp.where(lane_one == LANES - lead - tap, v[tap], row)
        steep = skewed(row, 2 * LANES)
        spot = down - across - lead
        matrix = jnp.where(jnp.logical_and(spot >= 0, spot < 2 * IH), steep, 0.0)
        warp_columns[b] = matrix.astype(BF16)
        warp_last[b, :LANES, :] = matrix[:LANES].astype(BF16)
        warp_last[b, LANES : LANES + HALF, :] = jnp.zeros((HALF, LANES), BF16)
        warp_last[b, LANES + HALF :, :] = matrix[LANES : LANES + HALF].astype(BF16)

    def relay(peer, side):
        span = pl.ds(KH, height)
        source = recv.at[span, pl.ds(0 if side == 0 else strip - LANES, LANES)]
        target = after.at[span, :] if side == 0 else before.at[span, :]
        return pltpu.make_async_remote_copy(
            src_ref=source,
            dst_ref=target,
            send_sem=relay_send.at[side],
            recv_sem=relay_recv.at[side],
            device_id={"band": peer},
            device_id_type=pl.DeviceIdType.MESH,
        )

    to_left = jnp.logical_and(me > 0, me != n // 2)
    to_right = jnp.logical_and(me < n - 1, me != n // 2 - 1)
    middle = jnp.logical_or(me == n // 2, me == n // 2 - 1)

    def pass_on():
        @pl.when(to_left)
        def _():
            relay(me - 1, 0).start()

        @pl.when(to_right)
        def _():
            relay(me + 1, 1).start()

    def take_ends():
        @pl.when(to_right)
        def _():
            relay(me + 1, 0).wait_recv()

        @pl.when(to_left)
        def _():
            relay(me - 1, 1).wait_recv()

        @pl.when(middle)
        def _():
            settle(end_recv, height - rows, LANES)
            settle(end_load, rows, LANES)

    def finish_relays():
        @pl.when(to_left)
        def _():
            relay(me - 1, 0).wait_send()

        @pl.when(to_right)
        def _():
            relay(me + 1, 1).wait_send()

        @pl.when(me != n // 2)
        def _():
            settle(end_send.at[1], rows, LANES)

        @pl.when(me != n // 2 - 1)
        def _():
            settle(end_send.at[0], rows, LANES)

    body = slice(KH, KH + height)
    upper = level // (LEVELS // 2)
    near_start = upper * half_rows
    far_start = half_rows - near_start

    def across_kernels(panels, mats, start, extent):
        body = pl.ds(pl.multiple_of(KH + start, KH), extent)
        if mats is outer_mats:
            windows = [ends[...]]
        else:
            windows = []
            for p in panels:
                if p == 0:
                    piece = recv[body, :LANES]
                    windows.append(jnp.concatenate([piece, piece], axis=1))
                else:
                    windows.append(recv[body, (p - 1) * LANES : (p + 1) * LANES])
        stacked = jnp.concatenate(windows, axis=0) if len(windows) > 1 else windows[0]
        for pair in range(NK // 2):
            result = jnp.dot(stacked, mats[pair], preferred_element_type=F32).astype(BF16)
            for i, p in enumerate(panels):
                for j in range(2):
                    crossed[2 * pair + j, body, p * LANES : (p + 1) * LANES] = result[
                        i * extent : (i + 1) * extent, j * LANES : (j + 1) * LANES
                    ]

    def gather_ends():
        lane = lax.broadcasted_iota(jnp.int32, (height, LANES), 1) < HALF
        ends[:, :LANES] = jnp.where(lane, after[body, :], before[body, :])
        ends[:, LANES:] = jnp.where(lane, recv[body, :LANES], recv[body, strip - LANES :])

    def render(panels):
        for g in range(0, len(panels), 2):
            group = panels[g : g + 2]
            start = 0
            for extent in split(height):
                total = jnp.zeros((extent, len(group) * LANES), F32)
                for k in range(NK):
                    window = slice(start, start + extent + 2 * KH)
                    pieces = [crossed[k, window, p * LANES : (p + 1) * LANES] for p in group]
                    field = jnp.dot(
                        row_mats[k, :extent, : extent + 2 * KH],
                        jnp.concatenate(pieces, axis=1) if len(pieces) > 1 else pieces[0],
                        preferred_element_type=F32,
                    )
                    total = total + weight_ref[k] * field * field
                into = slice(EDGE + start, EDGE + start + extent)
                for i, p in enumerate(group):
                    part = total[:, i * LANES : (i + 1) * LANES]
                    if p == tiles:
                        lanes = lax.broadcasted_iota(jnp.int32, (extent, LANES), 1)
                        column = me * strip + lanes - P_SIZE + jnp.where(
                            lanes < HALF, 0, strip - HALF
                        )
                        part = jnp.where(
                            jnp.logical_and(column >= 0, column < width), part, 0.0
                        ).astype(BF16)
                        intensity[into, strip:] = part
                        intensity[into, :LANES] = jnp.where(
                            lanes < LEAD, part, intensity[into, :LANES]
                        )
                    else:
                        intensity[into, p * LANES : (p + 1) * LANES] = part.astype(BF16)
                start += extent

    def halfway(panels):
        runs = []
        for p in sorted(panels):
            if runs and runs[-1][1] == p:
                runs[-1][1] = p + 1
            else:
                runs.append([p, p + 1])
        for b in range(count):
            for lo, hi in runs:
                partial[b * BLK : (b + 1) * BLK, lo * LANES : hi * LANES] = jnp.dot(
                    warp_rows[b, :, : BLK + 2 * EDGE],
                    intensity[b * BLK : (b + 1) * BLK + 2 * EDGE, lo * LANES : hi * LANES],
                    preferred_element_type=F32,
                ).astype(BF16)

    def finish(targets):
        targets = sorted(targets)
        common = [q for q in targets if q < tiles - 1]
        for b in range(count):
            own = slice(b * BLK, (b + 1) * BLK)
            care = care_ref[0, b].astype(F32)
            results = []
            if common:
                warped = jnp.dot(
                    jnp.concatenate(
                        [partial[own, q * LANES : (q + 2) * LANES] for q in common], axis=0
                    ),
                    warp_columns[b],
                    preferred_element_type=F32,
                )
                results += [(q, warped[i * BLK : (i + 1) * BLK]) for i, q in enumerate(common)]
            if tiles - 1 in targets:
                q = tiles - 1
                results.append(
                    (
                        q,
                        jnp.dot(
                            partial[own, q * LANES : (q + 2) * LANES], warp_last[b],
                            preferred_element_type=F32,
                        ),
                    )
                )
            for q, warped in results:
                measured = image[own, q * LANES : (q + 1) * LANES].astype(F32)
                diff[8 + b * BLK : 8 + (b + 1) * BLK, q * LANES : (q + 1) * LANES] = care * (
                    measured - warped
                )
        first = partial_sums[:8, :]
        second = partial_sums[8:, :]
        for q in targets:
            column = slice(q * LANES, (q + 1) * LANES)
            for start in range(0, height, BLK):
                around = diff[start : start + BLK + 16, column]
                value = around[8 : 8 + BLK] + 0.5 * (around[7 : 7 + BLK] + around[9 : 9 + BLK])
                filt[start : start + BLK, column] = value
                power = value * value
                for r in range(0, BLK, 8):
                    first = first + value[r : r + 8]
                    second = second + power[r : r + 8]
        partial_sums[:8, :] = first
        partial_sums[8:, :] = second

    loads[-1].wait()
    loads[-2].wait()
    fresh_of, seen, crossing = [], set(), set()
    for event in events:
        for lo, span in event:
            seen.update(range(lo, lo + span))
        fresh = [
            p for p in range(tiles)
            if p in seen and (p == 0 or p - 1 in seen) and p not in crossing
        ]
        crossing.update(fresh)
        fresh_of.append(fresh)

    def begin(e):
        settle_near(e)
        if fresh_of[e]:
            across_kernels(fresh_of[e], column_mats, near_start, half_rows)

    def settle_near(e):
        settle(recv_sem.at[e, 0], half_rows - rows, sizes[e])

    def settle_far(e):
        settle(recv_sem.at[e, 1], half_rows, sizes[e])

    settle_near(0)
    halves_due = []
    waiting, halves, done = [], set(), set()
    for e, event in enumerate(events):
        settle_far(e)
        if e == 0:
            pass_on()
            send_rest(True)
            if fresh_of[0]:
                across_kernels(fresh_of[0], column_mats, 0, height)
        elif fresh_of[e]:
            across_kernels(fresh_of[e], column_mats, far_start, half_rows)
        waiting += fresh_of[e]
        if e == min(1, len(events) - 1):
            take_ends()
            gather_ends()
            across_kernels([tiles], outer_mats, 0, height)
            waiting.append(tiles)
        render(waiting)
        if e == 0 and len(events) > 1:
            halves_due = waiting
            waiting = []
            begin(1)
            continue
        waiting = halves_due + waiting
        halves_due = []
        halfway(waiting)
        halves.update(waiting)
        waiting = []
        targets = {q for q in range(tiles) if q in halves and q + 1 in halves} - done
        finish(targets)
        done.update(targets)
        if e == 1:
            for later in range(2, len(events)):
                begin(later)

    stats_mine[0:1, :] = jnp.sum(partial_sums[:8, :], axis=0, keepdims=True)
    stats_mine[1:2, :] = jnp.sum(partial_sums[8:, :], axis=0, keepdims=True)

    def stat_to(peer):
        return pltpu.make_async_remote_copy(
            src_ref=stats_mine,
            dst_ref=stats_all.at[me],
            send_sem=stat_send,
            recv_sem=stat_recv,
            device_id={"band": peer},
            device_id_type=pl.DeviceIdType.MESH,
        )

    for peer in range(n):

        @pl.when(me != peer)
        def _():
            stat_to(jnp.int32(peer)).start()

    stats_all[me] = stats_mine[...]

    for e, columns in enumerate(sizes):
        settle(send_sem.at[e, 0], half_rows - rows, columns)
        settle(send_sem.at[e, 1], half_rows, columns)
    finish_relays()

    others = stats_all.at[pl.ds(0, n - 1)]
    pltpu.make_async_copy(others, others, stat_send).wait()
    pltpu.make_async_copy(others, others, stat_recv).wait()
    sums = jnp.sum(stats_all[...], axis=0)
    cells = height * width
    totals = jnp.sum(sums, axis=1, keepdims=True) / cells
    mean, power = totals[0:1], totals[1:2]
    scale = lax.rsqrt(power - mean * mean + epsilon)
    mean_ref[...] = jnp.broadcast_to(mean, (1, strip))
    for b in range(count):
        scale_ref[b : b + 1, :] = jnp.broadcast_to(care_ref[0, b].astype(F32) * scale, (1, strip))


def normalize(filtered, mean, scale, out, held, sem):
    height = filtered.shape[0]
    copies = []
    for at in range(0, height, PIECE):
        rows = slice(at, at + PIECE)
        b = at // BLK
        held[rows, :] = ((filtered[rows, :] - mean[...]) * scale[b : b + 1, :]).astype(BF16)
        copy = pltpu.make_async_copy(
            held.at[pl.ds(at, PIECE), :], out.at[pl.ds(at, PIECE), :], sem.at[at // PIECE]
        )
        copy.start()
        copies.append(copy)
    for copy in copies:
        copy.wait()


def on_device(
    design, row_taps, column_taps, kernel_weight, interp, block_shift, block_phase, care, image
):
    n = lax.axis_size("band")
    rows, width = design.shape
    height, strip = image.shape
    wide = strip + LANES
    count = height // BLK
    slots = len(plan(strip // LANES))
    tall = height + 2 * KH
    hbm = pl.BlockSpec(memory_space=pltpu.HBM)
    vmem = pl.BlockSpec(memory_space=pltpu.VMEM)
    filtered, mean, scale = pl.pallas_call(
        functools.partial(kernel, n, height, width),
        out_shape=(
            jax.ShapeDtypeStruct((height, strip), F32),
            jax.ShapeDtypeStruct((1, strip), F32),
            jax.ShapeDtypeStruct((count, strip), F32),
        ),
        in_specs=[hbm] * 9,
        out_specs=(vmem, vmem, vmem),
        scratch_shapes=[
            pltpu.SMEM((NK,), F32),
            pltpu.SMEM((2, 1, count), jnp.int32),
            pltpu.SMEM((2, 1, count), jnp.int32),
            pltpu.SMEM((1, count), jnp.int32),
            pltpu.VMEM(row_taps.shape, BF16),
            pltpu.VMEM(column_taps.shape, BF16),
            pltpu.VMEM(interp.shape[::-1], BF16),
            pltpu.VMEM((tall, strip), BF16),
            pltpu.VMEM((tall, LANES), BF16),
            pltpu.VMEM((tall, LANES), BF16),
            pltpu.VMEM((height, 2 * LANES), BF16),
            pltpu.VMEM((height, strip), BF16),
            pltpu.VMEM((NK, UNIT, 2 * LANES), BF16),
            pltpu.VMEM((NK // 2, 2 * LANES, 2 * LANES), BF16),
            pltpu.VMEM((NK // 2, 2 * LANES, 2 * LANES), BF16),
            pltpu.VMEM((count, BLK, 2 * LANES), BF16),
            pltpu.VMEM((count, 2 * LANES, LANES), BF16),
            pltpu.VMEM((count, 2 * LANES, LANES), BF16),
            pltpu.VMEM((NK, tall, wide), BF16),
            pltpu.VMEM((height + 2 * EDGE, wide), BF16),
            pltpu.VMEM((height, wide), BF16),
            pltpu.VMEM((height + 16, strip), F32),
            pltpu.VMEM((16, LANES), F32),
            pltpu.VMEM((2, LANES), F32),
            pltpu.VMEM((n, 2, LANES), F32),
            pltpu.SemaphoreType.DMA((slots, 2)),
            pltpu.SemaphoreType.DMA((slots, 2)),
            pltpu.SemaphoreType.DMA((2,)),
            pltpu.SemaphoreType.DMA((2,)),
            pltpu.SemaphoreType.DMA((2,)),
            pltpu.SemaphoreType.DMA,
            pltpu.SemaphoreType.DMA,
            pltpu.SemaphoreType.DMA,
            pltpu.SemaphoreType.DMA,
            pltpu.SemaphoreType.REGULAR,
            pltpu.SemaphoreType.REGULAR,
            pltpu.SemaphoreType.DMA((9,)),
        ],
        compiler_params=pltpu.CompilerParams(
            collective_id=0, has_side_effects=True, vmem_limit_bytes=48 * 1024 * 1024
        ),
    )(
        pin(kernel_weight),
        pin(jnp.transpose(block_shift, (0, 2, 1))),
        pin(jnp.transpose(block_phase, (0, 2, 1))),
        pin(care.T),
        pin(design),
        pin(row_taps),
        pin(column_taps),
        pin(interp.T),
        pin(image),
    )
    return pl.pallas_call(
        normalize,
        out_shape=jax.ShapeDtypeStruct((height, strip), BF16),
        in_specs=[vmem] * 3,
        out_specs=hbm,
        scratch_shapes=[
            pltpu.VMEM((height, strip), BF16),
            pltpu.SemaphoreType.DMA((height // PIECE,)),
        ],
        compiler_params=pltpu.CompilerParams(vmem_limit_bytes=8 * 1024 * 1024),
    )(filtered, mean, scale)


def solution(mesh):
    placed = (
        P(("swath", "band"), None),
        P(),
        P(),
        P(),
        P(),
        P(None, "swath", "band"),
        P(None, "swath", "band"),
        P("swath", "band"),
        P("swath", "band"),
    )
    return jax.shard_map(
        on_device, mesh=mesh, in_specs=placed, out_specs=P("swath", "band"), check_vma=False
    )
```

```python
import functools

import jax
import jax.numpy as jnp
from jax import lax
from jax.experimental import pallas as pl
from jax.experimental.pallas import tpu as pltpu
from jax.sharding import PartitionSpec as P

NK = 8
KH = 16
IH = 4
BLK = 128
P_SIZE = 28
LANES = 128
HALF = LANES // 2
EDGE = 32
PIECE = 64
UNIT = 144
REACH = 2 * KH + 1
LEAD = P_SIZE + KH
INNER = LANES - LEAD

LEVELS = 4
LATE = (3,)

epsilon = 1e-05

F32 = jnp.float32
BF16 = jnp.bfloat16


def pin(x):
    return pltpu.with_memory_space_constraint(x, pltpu.HBM)


def skewed(row, rows):
    base = jnp.broadcast_to(row, (rows, row.shape[1]))
    return pltpu.roll(base, 0, 1, stride=1, stride_axis=0)


def split(total):
    return [min(UNIT, total - at) for at in range(0, total, UNIT)]


def plan(tiles):
    if tiles < 4:
        return [[(0, tiles)]]
    events = [[(0, 1), (tiles - 1, 1)]]
    low, high = 1, tiles - 2
    left = True
    while low <= high:
        span = min(2, high - low + 1)
        events.append([(low if left else high - span + 1, span)])
        low, high = (low + span, high) if left else (low, high - span)
        left = not left
    return events


def kernel(
    n, height, width,
    weight_hbm, shift_hbm, phase_hbm, care_hbm,
    design_hbm, row_hbm, column_hbm, interp_hbm, image_hbm,
    filt, mean_ref, scale_ref,
    weight_ref, shift_ref, phase_ref, care_ref,
    row_ref, column_ref, interp_ref,
    recv, before, after, ends, image, row_mats, column_mats, outer_mats,
    warp_rows, warp_columns, warp_last, crossed, intensity, partial,
    diff, partial_sums, stats_mine, stats_all,
    send_sem, recv_sem, relay_send, relay_recv, end_send, end_recv, end_load, stat_send, stat_recv, two_away, three_away, load_sem,
):
    me = lax.axis_index("band")
    rows = height // n
    strip = width // n
    tiles = strip // LANES
    tall = height + 2 * KH
    count = height // BLK
    events = plan(tiles)

    barrier = pltpu.get_barrier_semaphore()

    mine = pl.ds(pl.multiple_of(KH + me * rows, rows), rows)
    loads = [
        pltpu.make_async_copy(source, target, load_sem.at[i])
        for i, (source, target) in enumerate(
            [
                (row_hbm, row_ref),
                (column_hbm, column_ref),
                (interp_hbm, interp_ref),
                (weight_hbm, weight_ref),
                (shift_hbm, shift_ref),
                (phase_hbm, phase_ref),
                (care_hbm, care_ref),
                (image_hbm, image),
                (
                    design_hbm.at[:, pl.ds(pl.multiple_of(me * strip, LANES), strip)],
                    recv.at[mine, :],
                ),
            ]
        )
    ]
    flips = {}
    bit = 1
    while bit < n:
        flips[bit] = bit * (1 - 2 * lax.rem(me // bit, 2))
        bit *= 2

    def partner(i):
        return me + sum(flip for bit, flip in flips.items() if i & bit)

    def send(peer, slot, lo, span, far):
        pltpu.make_async_remote_copy(
            src_ref=design_hbm.at[
                :, pl.ds(pl.multiple_of(peer * strip + lo * LANES, LANES), span * LANES)
            ],
            dst_ref=recv.at[mine, pl.ds(lo * LANES, span * LANES)],
            send_sem=send_sem.at[slot, far],
            recv_sem=recv_sem.at[slot, far],
            device_id={"band": peer},
            device_id_type=pl.DeviceIdType.MESH,
        ).start()

    def send_ends():
        for target, edge, tile in ((n // 2, before, -1), (n // 2 - 1, after, 0)):
            source = design_hbm.at[:, pl.ds((n // 2) * strip + tile * LANES, LANES)]
            place = edge.at[mine, :]

            @pl.when(me != target)
            def _():
                pltpu.make_async_remote_copy(
                    src_ref=source,
                    dst_ref=place,
                    send_sem=end_send.at[-tile],
                    recv_sem=end_recv,
                    device_id={"band": jnp.int32(target)},
                    device_id_type=pl.DeviceIdType.MESH,
                ).start()

            @pl.when(me == target)
            def _():
                pltpu.make_async_copy(source, place, end_load).start()

    def block(extent, columns):
        return recv.at[pl.ds(0, extent), pl.ds(0, columns)]

    def settle(sem, extent, columns):
        pltpu.make_async_copy(block(extent, columns), block(extent, columns), sem).wait()

    half_rows = height // 2
    sizes = [sum(span for _, span in event) * LANES for event in events]

    level = me // (n // LEVELS)
    inner = jnp.logical_and(level > 0, level < LEVELS - 1)
    outer = jnp.logical_not(inner)
    near = range(1, n // 2)
    second = range(n // 2, 3 * n // 4)
    third = range(3 * n // 4, n)

    def send_to(e, ids):
        for i in ids:
            for lo, span in events[e]:
                send(partner(i), e, lo, span, int(i >= n // 2))

    def tell(semaphore, i):
        pl.semaphore_signal(
            semaphore, inc=1, device_id={"band": partner(i)}, device_id_type=pl.DeviceIdType.MESH
        )

    for i in near:
        tell(barrier, i)

    @pl.when(inner)
    def _():
        for i in third:
            tell(barrier, i)

    for load in loads:
        load.start()
    pl.semaphore_wait(barrier, n // 2 - 1 + jnp.where(inner, n // 4, 0))
    early = range(1, min(2, len(events)))

    @pl.when(inner)
    def _():
        tell(two_away, n // LEVELS)
        tell(two_away, 3 * n // LEVELS)

    send_to(0, near)

    @pl.when(inner)
    def _():
        send_to(0, third)

        @pl.when(level == 1)
        def _():
            for e in early:
                send_to(e, third)

        pl.semaphore_wait(two_away, 1)
        tell(three_away, n // LEVELS)
        send_to(0, second)

    @pl.when(outer)
    def _():
        pl.semaphore_wait(two_away, 1)
        send_to(0, second)
        pl.semaphore_wait(three_away, 1)
        send_to(0, third)

    send_ends()
    for e in early:
        send_to(e, near)
        send_to(e, second)

        @pl.when(jnp.logical_not(level == 1))
        def _():
            send_to(e, third)

    def send_rest(late):
        if not late:
            for e in range(2, len(events)):
                send_to(e, near)
        for e in range(2, len(events)):
            if (e in LATE) == late:
                if not late:
                    send_to(e, range(n // 2, n))
                    continue

                @pl.when(inner)
                def _():
                    send_to(e, second)
                    send_to(e, third)

                @pl.when(outer)
                def _():
                    send_to(e, third)
                    send_to(e, second)

    send_rest(False)

    for k in range(NK):
        crossed[k, :KH, :] = jnp.zeros((KH, strip + LANES), BF16)
        crossed[k, KH + height :, :] = jnp.zeros((KH, strip + LANES), BF16)

    @pl.when(me == 0)
    def _():
        before[KH : KH + height, :] = jnp.zeros((height, LANES), BF16)

    @pl.when(me == n - 1)
    def _():
        after[KH : KH + height, :] = jnp.zeros((height, LANES), BF16)

    wide = strip + LANES
    intensity[:EDGE, :] = jnp.zeros((EDGE, wide), BF16)
    intensity[EDGE + height :, :] = jnp.zeros((EDGE, wide), BF16)
    diff[:8, :] = jnp.zeros((8, strip), F32)
    diff[8 + height :, :] = jnp.zeros((8, strip), F32)
    partial_sums[...] = jnp.zeros((16, LANES), F32)

    for load in loads[:-2]:
        load.wait()

    pad = jnp.zeros((NK, LANES - REACH), F32)
    row_table = jnp.concatenate([row_ref[...].astype(F32), pad, jnp.zeros((NK, LANES), F32)], axis=1)
    column_table = jnp.concatenate([column_ref[...].astype(F32), pad], axis=1)
    from_lane = lax.broadcasted_iota(jnp.int32, (LANES, LANES), 0)
    to_lane = lax.broadcasted_iota(jnp.int32, (LANES, LANES), 1)
    turned = jnp.where(lax.rem(2 * LANES - INNER - to_lane, LANES) == from_lane, 1.0, 0.0)
    backward = jnp.dot(
        column_table.astype(BF16), turned.astype(BF16), preferred_element_type=F32
    )
    backward_half = pltpu.roll(backward, HALF, 1)
    square = (2 * LANES, LANES)
    down = lax.broadcasted_iota(jnp.int32, square, 0)
    across = lax.broadcasted_iota(jnp.int32, square, 1)
    place = down - across - INNER
    inside = jnp.logical_and(place >= 0, place < REACH)
    low_lane = across < HALF
    place_far = lax.rem(down - across - INNER - HALF + 4 * LANES, 2 * LANES)
    inside_outer = jnp.where(low_lane, jnp.where(inside, 1, 0), jnp.where(place_far < REACH, 1, 0)) > 0
    for k in range(NK):
        row_mats[k] = skewed(row_table[k : k + 1], UNIT).astype(BF16)
        near = skewed(backward[k : k + 1], 2 * LANES)
        far = skewed(backward_half[k : k + 1], 2 * LANES)
        half = slice((k % 2) * LANES, (k % 2 + 1) * LANES)
        column_mats[k // 2, :, half] = jnp.where(inside, near, 0.0).astype(BF16)
        outer_mats[k // 2, :, half] = jnp.where(
            inside_outer, jnp.where(low_lane, near, far), 0.0
        ).astype(BF16)

    table = interp_ref[...].astype(F32)
    phases = lax.broadcasted_iota(jnp.int32, table.shape, 1)
    lane_wide = lax.broadcasted_iota(jnp.int32, (1, 2 * LANES), 1)
    lane_one = lax.broadcasted_iota(jnp.int32, (1, LANES), 1)

    def chosen(phase):
        row = jnp.sum(jnp.where(phases == phase, table, 0.0), axis=1, keepdims=True)
        return [row[t : t + 1] for t in range(2 * IH)]

    for b in range(count):
        u = chosen(phase_ref[0, 0, b])
        v = chosen(phase_ref[1, 0, b])
        lead = EDGE + 1 - IH + shift_ref[0, 0, b]
        row = jnp.zeros((1, 2 * LANES), F32)
        for tap in range(2 * IH):
            row = jnp.where(lane_wide == lead + tap, u[tap], row)
        warp_rows[b] = skewed(row, BLK).astype(BF16)
        lead = P_SIZE + 1 - IH + shift_ref[1, 0, b]
        row = jnp.zeros((1, LANES), F32)
        for tap in range(2 * IH):
            row = jnp.where(lane_one == LANES - lead - tap, v[tap], row)
        steep = skewed(row, 2 * LANES)
        spot = down - across - lead
        matrix = jnp.where(jnp.logical_and(spot >= 0, spot < 2 * IH), steep, 0.0)
        warp_columns[b] = matrix.astype(BF16)
        warp_last[b, :LANES, :] = matrix[:LANES].astype(BF16)
        warp_last[b, LANES : LANES + HALF, :] = jnp.zeros((HALF, LANES), BF16)
        warp_last[b, LANES + HALF :, :] = matrix[LANES : LANES + HALF].astype(BF16)

    def relay(peer, side):
        span = pl.ds(KH, height)
        source = recv.at[span, pl.ds(0 if side == 0 else strip - LANES, LANES)]
        target = after.at[span, :] if side == 0 else before.at[span, :]
        return pltpu.make_async_remote_copy(
            src_ref=source,
            dst_ref=target,
            send_sem=relay_send.at[side],
            recv_sem=relay_recv.at[side],
            device_id={"band": peer},
            device_id_type=pl.DeviceIdType.MESH,
        )

    to_left = jnp.logical_and(me > 0, me != n // 2)
    to_right = jnp.logical_and(me < n - 1, me != n // 2 - 1)
    middle = jnp.logical_or(me == n // 2, me == n // 2 - 1)

    def pass_on():
        @pl.when(to_left)
        def _():
            relay(me - 1, 0).start()

        @pl.when(to_right)
        def _():
            relay(me + 1, 1).start()

    def take_ends():
        @pl.when(to_right)
        def _():
            relay(me + 1, 0).wait_recv()

        @pl.when(to_left)
        def _():
            relay(me - 1, 1).wait_recv()

        @pl.when(middle)
        def _():
            settle(end_recv, height - rows, LANES)
            settle(end_load, rows, LANES)

    def finish_relays():
        @pl.when(to_left)
        def _():
            relay(me - 1, 0).wait_send()

        @pl.when(to_right)
        def _():
            relay(me + 1, 1).wait_send()

        @pl.when(me != n // 2)
        def _():
            settle(end_send.at[1], rows, LANES)

        @pl.when(me != n // 2 - 1)
        def _():
            settle(end_send.at[0], rows, LANES)

    body = slice(KH, KH + height)
    upper = level // (LEVELS // 2)
    near_start = upper * half_rows
    far_start = half_rows - near_start

    def across_kernels(panels, mats, start, extent):
        body = pl.ds(pl.multiple_of(KH + start, KH), extent)
        if mats is outer_mats:
            windows = [ends[...]]
        else:
            windows = []
            for p in panels:
                if p == 0:
                    piece = recv[body, :LANES]
                    windows.append(jnp.concatenate([piece, piece], axis=1))
                else:
                    windows.append(recv[body, (p - 1) * LANES : (p + 1) * LANES])
        stacked = jnp.concatenate(windows, axis=0) if len(windows) > 1 else windows[0]
        for pair in range(NK // 2):
            result = jnp.dot(stacked, mats[pair], preferred_element_type=F32).astype(BF16)
            for i, p in enumerate(panels):
                for j in range(2):
                    crossed[2 * pair + j, body, p * LANES : (p + 1) * LANES] = result[
                        i * extent : (i + 1) * extent, j * LANES : (j + 1) * LANES
                    ]

    def gather_ends():
        lane = lax.broadcasted_iota(jnp.int32, (height, LANES), 1) < HALF
        ends[:, :LANES] = jnp.where(lane, after[body, :], before[body, :])
        ends[:, LANES:] = jnp.where(lane, recv[body, :LANES], recv[body, strip - LANES :])

    def rows_at(start, extent):
        if isinstance(start, int):
            return slice(start, start + extent)
        return pl.ds(pl.multiple_of(start, KH), extent)

    def render(panels, first, total_rows):
        for g in range(0, len(panels), 2):
            group = panels[g : g + 2]
            at = 0
            for extent in split(total_rows):
                start = first + at
                total = jnp.zeros((extent, len(group) * LANES), F32)
                window = rows_at(start, extent + 2 * KH)
                for k in range(NK):
                    pieces = [crossed[k, window, p * LANES : (p + 1) * LANES] for p in group]
                    field = jnp.dot(
                        row_mats[k, :extent, : extent + 2 * KH],
                        jnp.concatenate(pieces, axis=1) if len(pieces) > 1 else pieces[0],
                        preferred_element_type=F32,
                    )
                    total = total + weight_ref[k] * field * field
                into = rows_at(EDGE + start, extent)
                for i, p in enumerate(group):
                    part = total[:, i * LANES : (i + 1) * LANES]
                    if p == tiles:
                        lanes = lax.broadcasted_iota(jnp.int32, (extent, LANES), 1)
                        column = me * strip + lanes - P_SIZE + jnp.where(
                            lanes < HALF, 0, strip - HALF
                        )
                        part = jnp.where(
                            jnp.logical_and(column >= 0, column < width), part, 0.0
                        ).astype(BF16)
                        intensity[into, strip:] = part
                        intensity[into, :LANES] = jnp.where(
                            lanes < LEAD, part, intensity[into, :LANES]
                        )
                    else:
                        intensity[into, p * LANES : (p + 1) * LANES] = part.astype(BF16)
                at += extent

    def halfway(panels):
        runs = []
        for p in sorted(panels):
            if runs and runs[-1][1] == p:
                runs[-1][1] = p + 1
            else:
                runs.append([p, p + 1])
        for b in range(count):
            for lo, hi in runs:
                partial[b * BLK : (b + 1) * BLK, lo * LANES : hi * LANES] = jnp.dot(
                    warp_rows[b, :, : BLK + 2 * EDGE],
                    intensity[b * BLK : (b + 1) * BLK + 2 * EDGE, lo * LANES : hi * LANES],
                    preferred_element_type=F32,
                ).astype(BF16)

    def finish(targets):
        targets = sorted(targets)
        common = [q for q in targets if q < tiles - 1]
        for b in range(count):
            own = slice(b * BLK, (b + 1) * BLK)
            care = care_ref[0, b].astype(F32)
            results = []
            if common:
                warped = jnp.dot(
                    jnp.concatenate(
                        [partial[own, q * LANES : (q + 2) * LANES] for q in common], axis=0
                    ),
                    warp_columns[b],
                    preferred_element_type=F32,
                )
                results += [(q, warped[i * BLK : (i + 1) * BLK]) for i, q in enumerate(common)]
            if tiles - 1 in targets:
                q = tiles - 1
                results.append(
                    (
                        q,
                        jnp.dot(
                            partial[own, q * LANES : (q + 2) * LANES], warp_last[b],
                            preferred_element_type=F32,
                        ),
                    )
                )
            for q, warped in results:
                measured = image[own, q * LANES : (q + 1) * LANES].astype(F32)
                diff[8 + b * BLK : 8 + (b + 1) * BLK, q * LANES : (q + 1) * LANES] = care * (
                    measured - warped
                )
        first = partial_sums[:8, :]
        second = partial_sums[8:, :]
        for q in targets:
            column = slice(q * LANES, (q + 1) * LANES)
            for start in range(0, height, BLK):
                around = diff[start : start + BLK + 16, column]
                value = around[8 : 8 + BLK] + 0.5 * (around[7 : 7 + BLK] + around[9 : 9 + BLK])
                filt[start : start + BLK, column] = value
                power = value * value
                for r in range(0, BLK, 8):
                    first = first + value[r : r + 8]
                    second = second + power[r : r + 8]
        partial_sums[:8, :] = first
        partial_sums[8:, :] = second

    loads[-1].wait()
    loads[-2].wait()
    fresh_of, seen, crossing = [], set(), set()
    for event in events:
        for lo, span in event:
            seen.update(range(lo, lo + span))
        fresh = [
            p for p in range(tiles)
            if p in seen and (p == 0 or p - 1 in seen) and p not in crossing
        ]
        crossing.update(fresh)
        fresh_of.append(fresh)

    def begin(e):
        settle_near(e)
        if fresh_of[e]:
            across_kernels(fresh_of[e], column_mats, near_start, half_rows)
            render(fresh_of[e], upper * (half_rows + KH), half_rows - KH)

    def settle_near(e):
        settle(recv_sem.at[e, 0], half_rows - rows, sizes[e])

    def settle_far(e):
        settle(recv_sem.at[e, 1], half_rows, sizes[e])

    settle_near(0)
    halves_due = []
    waiting, halves, done = [], set(), set()
    for e, event in enumerate(events):
        settle_far(e)
        if e == 0:
            pass_on()
            send_rest(True)
            if fresh_of[0]:
                across_kernels(fresh_of[0], column_mats, 0, height)
                render(fresh_of[0], 0, height)
        elif fresh_of[e]:
            across_kernels(fresh_of[e], column_mats, far_start, half_rows)
            render(fresh_of[e], (1 - upper) * (half_rows - KH), half_rows + KH)
        waiting += fresh_of[e]
        if e == min(1, len(events) - 1):
            take_ends()
            gather_ends()
            across_kernels([tiles], outer_mats, 0, height)
            render([tiles], 0, height)
            waiting.append(tiles)
        if e == 0 and len(events) > 1:
            halves_due = waiting
            waiting = []
            for later in range(1, len(events)):
                begin(later)
            continue
        waiting = halves_due + waiting
        halves_due = []
        halfway(waiting)
        halves.update(waiting)
        waiting = []
        targets = {q for q in range(tiles) if q in halves and q + 1 in halves} - done
        finish(targets)
        done.update(targets)

    stats_mine[0:1, :] = jnp.sum(partial_sums[:8, :], axis=0, keepdims=True)
    stats_mine[1:2, :] = jnp.sum(partial_sums[8:, :], axis=0, keepdims=True)

    def stat_to(peer):
        return pltpu.make_async_remote_copy(
            src_ref=stats_mine,
            dst_ref=stats_all.at[me],
            send_sem=stat_send,
            recv_sem=stat_recv,
            device_id={"band": peer},
            device_id_type=pl.DeviceIdType.MESH,
        )

    for peer in range(n):

        @pl.when(me != peer)
        def _():
            stat_to(jnp.int32(peer)).start()

    stats_all[me] = stats_mine[...]

    for e, columns in enumerate(sizes):
        settle(send_sem.at[e, 0], half_rows - rows, columns)
        settle(send_sem.at[e, 1], half_rows, columns)
    finish_relays()

    others = stats_all.at[pl.ds(0, n - 1)]
    pltpu.make_async_copy(others, others, stat_send).wait()
    pltpu.make_async_copy(others, others, stat_recv).wait()
    sums = jnp.sum(stats_all[...], axis=0)
    cells = height * width
    totals = jnp.sum(sums, axis=1, keepdims=True) / cells
    mean, power = totals[0:1], totals[1:2]
    scale = lax.rsqrt(power - mean * mean + epsilon)
    mean_ref[...] = jnp.broadcast_to(mean, (1, strip))
    for b in range(count):
        scale_ref[b : b + 1, :] = jnp.broadcast_to(care_ref[0, b].astype(F32) * scale, (1, strip))


def normalize(filtered, mean, scale, out, held, sem):
    height = filtered.shape[0]
    copies = []
    for at in range(0, height, PIECE):
        rows = slice(at, at + PIECE)
        b = at // BLK
        held[rows, :] = ((filtered[rows, :] - mean[...]) * scale[b : b + 1, :]).astype(BF16)
        copy = pltpu.make_async_copy(
            held.at[pl.ds(at, PIECE), :], out.at[pl.ds(at, PIECE), :], sem.at[at // PIECE]
        )
        copy.start()
        copies.append(copy)
    for copy in copies:
        copy.wait()


def on_device(
    design, row_taps, column_taps, kernel_weight, interp, block_shift, block_phase, care, image
):
    n = lax.axis_size("band")
    rows, width = design.shape
    height, strip = image.shape
    wide = strip + LANES
    count = height // BLK
    slots = len(plan(strip // LANES))
    tall = height + 2 * KH
    hbm = pl.BlockSpec(memory_space=pltpu.HBM)
    vmem = pl.BlockSpec(memory_space=pltpu.VMEM)
    filtered, mean, scale = pl.pallas_call(
        functools.partial(kernel, n, height, width),
        out_shape=(
            jax.ShapeDtypeStruct((height, strip), F32),
            jax.ShapeDtypeStruct((1, strip), F32),
            jax.ShapeDtypeStruct((count, strip), F32),
        ),
        in_specs=[hbm] * 9,
        out_specs=(vmem, vmem, vmem),
        scratch_shapes=[
            pltpu.SMEM((NK,), F32),
            pltpu.SMEM((2, 1, count), jnp.int32),
            pltpu.SMEM((2, 1, count), jnp.int32),
            pltpu.SMEM((1, count), jnp.int32),
            pltpu.VMEM(row_taps.shape, BF16),
            pltpu.VMEM(column_taps.shape, BF16),
            pltpu.VMEM(interp.shape[::-1], BF16),
            pltpu.VMEM((tall, strip), BF16),
            pltpu.VMEM((tall, LANES), BF16),
            pltpu.VMEM((tall, LANES), BF16),
            pltpu.VMEM((height, 2 * LANES), BF16),
            pltpu.VMEM((height, strip), BF16),
            pltpu.VMEM((NK, UNIT, 2 * LANES), BF16),
            pltpu.VMEM((NK // 2, 2 * LANES, 2 * LANES), BF16),
            pltpu.VMEM((NK // 2, 2 * LANES, 2 * LANES), BF16),
            pltpu.VMEM((count, BLK, 2 * LANES), BF16),
            pltpu.VMEM((count, 2 * LANES, LANES), BF16),
            pltpu.VMEM((count, 2 * LANES, LANES), BF16),
            pltpu.VMEM((NK, tall, wide), BF16),
            pltpu.VMEM((height + 2 * EDGE, wide), BF16),
            pltpu.VMEM((height, wide), BF16),
            pltpu.VMEM((height + 16, strip), F32),
            pltpu.VMEM((16, LANES), F32),
            pltpu.VMEM((2, LANES), F32),
            pltpu.VMEM((n, 2, LANES), F32),
            pltpu.SemaphoreType.DMA((slots, 2)),
            pltpu.SemaphoreType.DMA((slots, 2)),
            pltpu.SemaphoreType.DMA((2,)),
            pltpu.SemaphoreType.DMA((2,)),
            pltpu.SemaphoreType.DMA((2,)),
            pltpu.SemaphoreType.DMA,
            pltpu.SemaphoreType.DMA,
            pltpu.SemaphoreType.DMA,
            pltpu.SemaphoreType.DMA,
            pltpu.SemaphoreType.REGULAR,
            pltpu.SemaphoreType.REGULAR,
            pltpu.SemaphoreType.DMA((9,)),
        ],
        compiler_params=pltpu.CompilerParams(
            collective_id=0, has_side_effects=True, vmem_limit_bytes=48 * 1024 * 1024
        ),
    )(
        pin(kernel_weight),
        pin(jnp.transpose(block_shift, (0, 2, 1))),
        pin(jnp.transpose(block_phase, (0, 2, 1))),
        pin(care.T),
        pin(design),
        pin(row_taps),
        pin(column_taps),
        pin(interp.T),
        pin(image),
    )
    return pl.pallas_call(
        normalize,
        out_shape=jax.ShapeDtypeStruct((height, strip), BF16),
        in_specs=[vmem] * 3,
        out_specs=hbm,
        scratch_shapes=[
            pltpu.VMEM((height, strip), BF16),
            pltpu.SemaphoreType.DMA((height // PIECE,)),
        ],
        compiler_params=pltpu.CompilerParams(vmem_limit_bytes=8 * 1024 * 1024),
    )(filtered, mean, scale)


def solution(mesh):
    placed = (
        P(("swath", "band"), None),
        P(),
        P(),
        P(),
        P(),
        P(None, "swath", "band"),
        P(None, "swath", "band"),
        P("swath", "band"),
        P("swath", "band"),
    )
    return jax.shard_map(
        on_device, mesh=mesh, in_specs=placed, out_specs=P("swath", "band"), check_vma=False
    )
```

```python
import functools

import jax
import jax.numpy as jnp
from jax import lax
from jax.experimental import pallas as pl
from jax.experimental.pallas import tpu as pltpu
from jax.sharding import PartitionSpec as P

NK = 8
KH = 16
IH = 4
BLK = 128
P_SIZE = 28
LANES = 128
HALF = LANES // 2
EDGE = 32
PIECE = 64
UNIT = 144
REACH = 2 * KH + 1
LEAD = P_SIZE + KH
INNER = LANES - LEAD

LEVELS = 4
LATE = ()

epsilon = 1e-05

F32 = jnp.float32
BF16 = jnp.bfloat16


def pin(x):
    return pltpu.with_memory_space_constraint(x, pltpu.HBM)


def skewed(row, rows):
    base = jnp.broadcast_to(row, (rows, row.shape[1]))
    return pltpu.roll(base, 0, 1, stride=1, stride_axis=0)


def split(total):
    return [min(UNIT, total - at) for at in range(0, total, UNIT)]


def plan(tiles):
    if tiles < 4:
        return [[(0, tiles)]]
    events = [[(0, 1), (tiles - 1, 1)]]
    low, high = 1, tiles - 2
    left = True
    while low <= high:
        span = min(2, high - low + 1)
        events.append([(low if left else high - span + 1, span)])
        low, high = (low + span, high) if left else (low, high - span)
        left = not left
    return events


def kernel(
    n, height, width,
    weight_hbm, shift_hbm, phase_hbm, care_hbm,
    design_hbm, row_hbm, column_hbm, interp_hbm, image_hbm,
    filt, mean_ref, scale_ref,
    weight_ref, shift_ref, phase_ref, care_ref,
    row_ref, column_ref, interp_ref,
    recv, before, after, ends, image, row_mats, column_mats, outer_mats,
    warp_rows, warp_columns, warp_last, crossed, intensity, partial,
    diff, partial_sums, stats_mine, stats_all,
    send_sem, recv_sem, relay_send, relay_recv, end_send, end_recv, end_load, stat_send, stat_recv, two_away, three_away, load_sem,
):
    me = lax.axis_index("band")
    rows = height // n
    strip = width // n
    tiles = strip // LANES
    tall = height + 2 * KH
    count = height // BLK
    events = plan(tiles)

    barrier = pltpu.get_barrier_semaphore()

    mine = pl.ds(pl.multiple_of(KH + me * rows, rows), rows)
    loads = [
        pltpu.make_async_copy(source, target, load_sem.at[i])
        for i, (source, target) in enumerate(
            [
                (row_hbm, row_ref),
                (column_hbm, column_ref),
                (interp_hbm, interp_ref),
                (weight_hbm, weight_ref),
                (shift_hbm, shift_ref),
                (phase_hbm, phase_ref),
                (care_hbm, care_ref),
                (image_hbm, image),
                (
                    design_hbm.at[:, pl.ds(pl.multiple_of(me * strip, LANES), strip)],
                    recv.at[mine, :],
                ),
            ]
        )
    ]
    flips = {}
    bit = 1
    while bit < n:
        flips[bit] = bit * (1 - 2 * lax.rem(me // bit, 2))
        bit *= 2

    def partner(i):
        return me + sum(flip for bit, flip in flips.items() if i & bit)

    def send(peer, slot, lo, span, far):
        pltpu.make_async_remote_copy(
            src_ref=design_hbm.at[
                :, pl.ds(pl.multiple_of(peer * strip + lo * LANES, LANES), span * LANES)
            ],
            dst_ref=recv.at[mine, pl.ds(lo * LANES, span * LANES)],
            send_sem=send_sem.at[slot, far],
            recv_sem=recv_sem.at[slot, far],
            device_id={"band": peer},
            device_id_type=pl.DeviceIdType.MESH,
        ).start()

    def send_ends():
        for target, edge, tile in ((n // 2, before, -1), (n // 2 - 1, after, 0)):
            source = design_hbm.at[:, pl.ds((n // 2) * strip + tile * LANES, LANES)]
            place = edge.at[mine, :]

            @pl.when(me != target)
            def _():
                pltpu.make_async_remote_copy(
                    src_ref=source,
                    dst_ref=place,
                    send_sem=end_send.at[-tile],
                    recv_sem=end_recv,
                    device_id={"band": jnp.int32(target)},
                    device_id_type=pl.DeviceIdType.MESH,
                ).start()

            @pl.when(me == target)
            def _():
                pltpu.make_async_copy(source, place, end_load).start()

    def block(extent, columns):
        return recv.at[pl.ds(0, extent), pl.ds(0, columns)]

    def settle(sem, extent, columns):
        pltpu.make_async_copy(block(extent, columns), block(extent, columns), sem).wait()

    half_rows = height // 2
    sizes = [sum(span for _, span in event) * LANES for event in events]

    level = me // (n // LEVELS)
    inner = jnp.logical_and(level > 0, level < LEVELS - 1)
    outer = jnp.logical_not(inner)
    near = range(1, n // 2)
    second = range(n // 2, 3 * n // 4)
    third = range(3 * n // 4, n)

    def send_to(e, ids):
        for i in ids:
            for lo, span in events[e]:
                send(partner(i), e, lo, span, int(i >= n // 2))

    def tell(semaphore, i):
        pl.semaphore_signal(
            semaphore, inc=1, device_id={"band": partner(i)}, device_id_type=pl.DeviceIdType.MESH
        )

    for i in near:
        tell(barrier, i)

    @pl.when(inner)
    def _():
        for i in third:
            tell(barrier, i)

    for load in loads:
        load.start()
    pl.semaphore_wait(barrier, n // 2 - 1 + jnp.where(inner, n // 4, 0))
    early = range(1, min(2, len(events)))

    @pl.when(inner)
    def _():
        tell(two_away, n // LEVELS)
        tell(two_away, 3 * n // LEVELS)

    send_to(0, near)

    @pl.when(inner)
    def _():
        send_to(0, third)

        @pl.when(level == 1)
        def _():
            for e in early:
                send_to(e, third)

        pl.semaphore_wait(two_away, 1)
        tell(three_away, n // LEVELS)
        send_to(0, second)

    @pl.when(outer)
    def _():
        pl.semaphore_wait(two_away, 1)
        send_to(0, second)
        pl.semaphore_wait(three_away, 1)
        send_to(0, third)

    send_ends()
    for e in early:
        send_to(e, near)
        send_to(e, second)

        @pl.when(jnp.logical_not(level == 1))
        def _():
            send_to(e, third)

    def send_rest(late):
        if not late:
            for e in range(2, len(events)):
                send_to(e, near)
        for e in range(2, len(events)):
            if (e in LATE) == late:
                if not late:
                    send_to(e, range(n // 2, n))
                    continue

                @pl.when(inner)
                def _():
                    send_to(e, second)
                    send_to(e, third)

                @pl.when(outer)
                def _():
                    send_to(e, third)
                    send_to(e, second)

    send_rest(False)

    for k in range(NK):
        crossed[k, :KH, :] = jnp.zeros((KH, strip + LANES), BF16)
        crossed[k, KH + height :, :] = jnp.zeros((KH, strip + LANES), BF16)

    @pl.when(me == 0)
    def _():
        before[KH : KH + height, :] = jnp.zeros((height, LANES), BF16)

    @pl.when(me == n - 1)
    def _():
        after[KH : KH + height, :] = jnp.zeros((height, LANES), BF16)

    wide = strip + LANES
    intensity[:EDGE, :] = jnp.zeros((EDGE, wide), BF16)
    intensity[EDGE + height :, :] = jnp.zeros((EDGE, wide), BF16)
    diff[:8, :] = jnp.zeros((8, strip), F32)
    diff[8 + height :, :] = jnp.zeros((8, strip), F32)
    partial_sums[...] = jnp.zeros((16, LANES), F32)

    for load in loads[:-2]:
        load.wait()

    pad = jnp.zeros((NK, LANES - REACH), F32)
    row_table = jnp.concatenate([row_ref[...].astype(F32), pad, jnp.zeros((NK, LANES), F32)], axis=1)
    column_table = jnp.concatenate([column_ref[...].astype(F32), pad], axis=1)
    from_lane = lax.broadcasted_iota(jnp.int32, (LANES, LANES), 0)
    to_lane = lax.broadcasted_iota(jnp.int32, (LANES, LANES), 1)
    turned = jnp.where(lax.rem(2 * LANES - INNER - to_lane, LANES) == from_lane, 1.0, 0.0)
    backward = jnp.dot(
        column_table.astype(BF16), turned.astype(BF16), preferred_element_type=F32
    )
    backward_half = pltpu.roll(backward, HALF, 1)
    square = (2 * LANES, LANES)
    down = lax.broadcasted_iota(jnp.int32, square, 0)
    across = lax.broadcasted_iota(jnp.int32, square, 1)
    place = down - across - INNER
    inside = jnp.logical_and(place >= 0, place < REACH)
    low_lane = across < HALF
    place_far = lax.rem(down - across - INNER - HALF + 4 * LANES, 2 * LANES)
    inside_outer = jnp.where(low_lane, jnp.where(inside, 1, 0), jnp.where(place_far < REACH, 1, 0)) > 0
    for k in range(NK):
        row_mats[k] = skewed(row_table[k : k + 1], UNIT).astype(BF16)
        near = skewed(backward[k : k + 1], 2 * LANES)
        far = skewed(backward_half[k : k + 1], 2 * LANES)
        half = slice((k % 2) * LANES, (k % 2 + 1) * LANES)
        column_mats[k // 2, :, half] = jnp.where(inside, near, 0.0).astype(BF16)
        outer_mats[k // 2, :, half] = jnp.where(
            inside_outer, jnp.where(low_lane, near, far), 0.0
        ).astype(BF16)

    table = interp_ref[...].astype(F32)
    phases = lax.broadcasted_iota(jnp.int32, table.shape, 1)
    lane_wide = lax.broadcasted_iota(jnp.int32, (1, 2 * LANES), 1)
    lane_one = lax.broadcasted_iota(jnp.int32, (1, LANES), 1)

    def chosen(phase):
        row = jnp.sum(jnp.where(phases == phase, table, 0.0), axis=1, keepdims=True)
        return [row[t : t + 1] for t in range(2 * IH)]

    for b in range(count):
        u = chosen(phase_ref[0, 0, b])
        v = chosen(phase_ref[1, 0, b])
        lead = EDGE + 1 - IH + shift_ref[0, 0, b]
        row = jnp.zeros((1, 2 * LANES), F32)
        for tap in range(2 * IH):
            row = jnp.where(lane_wide == lead + tap, u[tap], row)
        warp_rows[b] = skewed(row, BLK).astype(BF16)
        lead = P_SIZE + 1 - IH + shift_ref[1, 0, b]
        row = jnp.zeros((1, LANES), F32)
        for tap in range(2 * IH):
            row = jnp.where(lane_one == LANES - lead - tap, v[tap], row)
        steep = skewed(row, 2 * LANES)
        spot = down - across - lead
        matrix = jnp.where(jnp.logical_and(spot >= 0, spot < 2 * IH), steep, 0.0)
        warp_columns[b] = matrix.astype(BF16)
        warp_last[b, :LANES, :] = matrix[:LANES].astype(BF16)
        warp_last[b, LANES : LANES + HALF, :] = jnp.zeros((HALF, LANES), BF16)
        warp_last[b, LANES + HALF :, :] = matrix[LANES : LANES + HALF].astype(BF16)

    def relay(peer, side):
        span = pl.ds(KH, height)
        source = recv.at[span, pl.ds(0 if side == 0 else strip - LANES, LANES)]
        target = after.at[span, :] if side == 0 else before.at[span, :]
        return pltpu.make_async_remote_copy(
            src_ref=source,
            dst_ref=target,
            send_sem=relay_send.at[side],
            recv_sem=relay_recv.at[side],
            device_id={"band": peer},
            device_id_type=pl.DeviceIdType.MESH,
        )

    to_left = jnp.logical_and(me > 0, me != n // 2)
    to_right = jnp.logical_and(me < n - 1, me != n // 2 - 1)
    middle = jnp.logical_or(me == n // 2, me == n // 2 - 1)

    def pass_on():
        @pl.when(to_left)
        def _():
            relay(me - 1, 0).start()

        @pl.when(to_right)
        def _():
            relay(me + 1, 1).start()

    def take_ends():
        @pl.when(to_right)
        def _():
            relay(me + 1, 0).wait_recv()

        @pl.when(to_left)
        def _():
            relay(me - 1, 1).wait_recv()

        @pl.when(middle)
        def _():
            settle(end_recv, height - rows, LANES)
            settle(end_load, rows, LANES)

    def finish_relays():
        @pl.when(to_left)
        def _():
            relay(me - 1, 0).wait_send()

        @pl.when(to_right)
        def _():
            relay(me + 1, 1).wait_send()

        @pl.when(me != n // 2)
        def _():
            settle(end_send.at[1], rows, LANES)

        @pl.when(me != n // 2 - 1)
        def _():
            settle(end_send.at[0], rows, LANES)

    body = slice(KH, KH + height)
    upper = level // (LEVELS // 2)
    near_start = upper * half_rows
    far_start = half_rows - near_start

    def across_kernels(panels, mats, start, extent):
        body = pl.ds(pl.multiple_of(KH + start, KH), extent)
        if mats is outer_mats:
            windows = [ends[...]]
        else:
            windows = []
            for p in panels:
                if p == 0:
                    piece = recv[body, :LANES]
                    windows.append(jnp.concatenate([piece, piece], axis=1))
                else:
                    windows.append(recv[body, (p - 1) * LANES : (p + 1) * LANES])
        stacked = jnp.concatenate(windows, axis=0) if len(windows) > 1 else windows[0]
        for pair in range(NK // 2):
            result = jnp.dot(stacked, mats[pair], preferred_element_type=F32).astype(BF16)
            for i, p in enumerate(panels):
                for j in range(2):
                    crossed[2 * pair + j, body, p * LANES : (p + 1) * LANES] = result[
                        i * extent : (i + 1) * extent, j * LANES : (j + 1) * LANES
                    ]

    def gather_ends():
        lane = lax.broadcasted_iota(jnp.int32, (height, LANES), 1) < HALF
        ends[:, :LANES] = jnp.where(lane, after[body, :], before[body, :])
        ends[:, LANES:] = jnp.where(lane, recv[body, :LANES], recv[body, strip - LANES :])

    def rows_at(start, extent):
        if isinstance(start, int):
            return slice(start, start + extent)
        return pl.ds(pl.multiple_of(start, KH), extent)

    def render(panels, first, total_rows):
        for g in range(0, len(panels), 2):
            group = panels[g : g + 2]
            at = 0
            for extent in split(total_rows):
                start = first + at
                total = jnp.zeros((extent, len(group) * LANES), F32)
                window = rows_at(start, extent + 2 * KH)
                for k in range(NK):
                    pieces = [crossed[k, window, p * LANES : (p + 1) * LANES] for p in group]
                    field = jnp.dot(
                        row_mats[k, :extent, : extent + 2 * KH],
                        jnp.concatenate(pieces, axis=1) if len(pieces) > 1 else pieces[0],
                        preferred_element_type=F32,
                    )
                    total = total + weight_ref[k] * field * field
                into = rows_at(EDGE + start, extent)
                for i, p in enumerate(group):
                    part = total[:, i * LANES : (i + 1) * LANES]
                    if p == tiles:
                        lanes = lax.broadcasted_iota(jnp.int32, (extent, LANES), 1)
                        column = me * strip + lanes - P_SIZE + jnp.where(
                            lanes < HALF, 0, strip - HALF
                        )
                        part = jnp.where(
                            jnp.logical_and(column >= 0, column < width), part, 0.0
                        ).astype(BF16)
                        intensity[into, strip:] = part
                        intensity[into, :LANES] = jnp.where(
                            lanes < LEAD, part, intensity[into, :LANES]
                        )
                    else:
                        intensity[into, p * LANES : (p + 1) * LANES] = part.astype(BF16)
                at += extent

    def halfway(panels):
        runs = []
        for p in sorted(panels):
            if runs and runs[-1][1] == p:
                runs[-1][1] = p + 1
            else:
                runs.append([p, p + 1])
        for b in range(count):
            for lo, hi in runs:
                partial[b * BLK : (b + 1) * BLK, lo * LANES : hi * LANES] = jnp.dot(
                    warp_rows[b, :, : BLK + 2 * EDGE],
                    intensity[b * BLK : (b + 1) * BLK + 2 * EDGE, lo * LANES : hi * LANES],
                    preferred_element_type=F32,
                ).astype(BF16)

    def finish(targets):
        targets = sorted(targets)
        common = [q for q in targets if q < tiles - 1]
        for b in range(count):
            own = slice(b * BLK, (b + 1) * BLK)
            care = care_ref[0, b].astype(F32)
            results = []
            if common:
                warped = jnp.dot(
                    jnp.concatenate(
                        [partial[own, q * LANES : (q + 2) * LANES] for q in common], axis=0
                    ),
                    warp_columns[b],
                    preferred_element_type=F32,
                )
                results += [(q, warped[i * BLK : (i + 1) * BLK]) for i, q in enumerate(common)]
            if tiles - 1 in targets:
                q = tiles - 1
                results.append(
                    (
                        q,
                        jnp.dot(
                            partial[own, q * LANES : (q + 2) * LANES], warp_last[b],
                            preferred_element_type=F32,
                        ),
                    )
                )
            for q, warped in results:
                measured = image[own, q * LANES : (q + 1) * LANES].astype(F32)
                diff[8 + b * BLK : 8 + (b + 1) * BLK, q * LANES : (q + 1) * LANES] = care * (
                    measured - warped
                )
        first = partial_sums[:8, :]
        second = partial_sums[8:, :]
        for q in targets:
            column = slice(q * LANES, (q + 1) * LANES)
            for start in range(0, height, BLK):
                around = diff[start : start + BLK + 16, column]
                value = around[8 : 8 + BLK] + 0.5 * (around[7 : 7 + BLK] + around[9 : 9 + BLK])
                filt[start : start + BLK, column] = value
                power = value * value
                for r in range(0, BLK, 8):
                    first = first + value[r : r + 8]
                    second = second + power[r : r + 8]
        partial_sums[:8, :] = first
        partial_sums[8:, :] = second

    loads[-1].wait()
    loads[-2].wait()
    fresh_of, seen, crossing = [], set(), set()
    for event in events:
        for lo, span in event:
            seen.update(range(lo, lo + span))
        fresh = [
            p for p in range(tiles)
            if p in seen and (p == 0 or p - 1 in seen) and p not in crossing
        ]
        crossing.update(fresh)
        fresh_of.append(fresh)

    def begin(e):
        settle_near(e)
        if fresh_of[e]:
            across_kernels(fresh_of[e], column_mats, near_start, half_rows)
            render(fresh_of[e], upper * (half_rows + KH), half_rows - KH)

    def settle_near(e):
        settle(recv_sem.at[e, 0], half_rows - rows, sizes[e])

    def settle_far(e):
        settle(recv_sem.at[e, 1], half_rows, sizes[e])

    settle_near(0)
    halves_due = []
    waiting, halves, done = [], set(), set()
    for e, event in enumerate(events):
        settle_far(e)
        if e == 0:
            pass_on()
            send_rest(True)
            if fresh_of[0]:
                across_kernels(fresh_of[0], column_mats, 0, height)
                render(fresh_of[0], 0, height)
        elif fresh_of[e]:
            across_kernels(fresh_of[e], column_mats, far_start, half_rows)
            render(fresh_of[e], (1 - upper) * (half_rows - KH), half_rows + KH)
        waiting += fresh_of[e]
        if e == min(1, len(events) - 1):
            take_ends()
            gather_ends()
            across_kernels([tiles], outer_mats, 0, height)
            render([tiles], 0, height)
            waiting.append(tiles)
        if e == 0 and len(events) > 1:
            halves_due = waiting
            waiting = []
            for later in range(1, len(events)):
                begin(later)
            continue
        waiting = halves_due + waiting
        halves_due = []
        halfway(waiting)
        halves.update(waiting)
        waiting = []
        targets = {q for q in range(tiles) if q in halves and q + 1 in halves} - done
        finish(targets)
        done.update(targets)

    stats_mine[0:1, :] = jnp.sum(partial_sums[:8, :], axis=0, keepdims=True)
    stats_mine[1:2, :] = jnp.sum(partial_sums[8:, :], axis=0, keepdims=True)

    def stat_to(peer):
        return pltpu.make_async_remote_copy(
            src_ref=stats_mine,
            dst_ref=stats_all.at[me],
            send_sem=stat_send,
            recv_sem=stat_recv,
            device_id={"band": peer},
            device_id_type=pl.DeviceIdType.MESH,
        )

    for peer in range(n):

        @pl.when(me != peer)
        def _():
            stat_to(jnp.int32(peer)).start()

    stats_all[me] = stats_mine[...]

    for e, columns in enumerate(sizes):
        settle(send_sem.at[e, 0], half_rows - rows, columns)
        settle(send_sem.at[e, 1], half_rows, columns)
    finish_relays()

    others = stats_all.at[pl.ds(0, n - 1)]
    pltpu.make_async_copy(others, others, stat_send).wait()
    pltpu.make_async_copy(others, others, stat_recv).wait()
    sums = jnp.sum(stats_all[...], axis=0)
    cells = height * width
    totals = jnp.sum(sums, axis=1, keepdims=True) / cells
    mean, power = totals[0:1], totals[1:2]
    scale = lax.rsqrt(power - mean * mean + epsilon)
    mean_ref[...] = jnp.broadcast_to(mean, (1, strip))
    for b in range(count):
        scale_ref[b : b + 1, :] = jnp.broadcast_to(care_ref[0, b].astype(F32) * scale, (1, strip))


def normalize(filtered, mean, scale, out, held, sem):
    height = filtered.shape[0]
    copies = []
    for at in range(0, height, PIECE):
        rows = slice(at, at + PIECE)
        b = at // BLK
        held[rows, :] = ((filtered[rows, :] - mean[...]) * scale[b : b + 1, :]).astype(BF16)
        copy = pltpu.make_async_copy(
            held.at[pl.ds(at, PIECE), :], out.at[pl.ds(at, PIECE), :], sem.at[at // PIECE]
        )
        copy.start()
        copies.append(copy)
    for copy in copies:
        copy.wait()


def on_device(
    design, row_taps, column_taps, kernel_weight, interp, block_shift, block_phase, care, image
):
    n = lax.axis_size("band")
    rows, width = design.shape
    height, strip = image.shape
    wide = strip + LANES
    count = height // BLK
    slots = len(plan(strip // LANES))
    tall = height + 2 * KH
    hbm = pl.BlockSpec(memory_space=pltpu.HBM)
    vmem = pl.BlockSpec(memory_space=pltpu.VMEM)
    filtered, mean, scale = pl.pallas_call(
        functools.partial(kernel, n, height, width),
        out_shape=(
            jax.ShapeDtypeStruct((height, strip), F32),
            jax.ShapeDtypeStruct((1, strip), F32),
            jax.ShapeDtypeStruct((count, strip), F32),
        ),
        in_specs=[hbm] * 9,
        out_specs=(vmem, vmem, vmem),
        scratch_shapes=[
            pltpu.SMEM((NK,), F32),
            pltpu.SMEM((2, 1, count), jnp.int32),
            pltpu.SMEM((2, 1, count), jnp.int32),
            pltpu.SMEM((1, count), jnp.int32),
            pltpu.VMEM(row_taps.shape, BF16),
            pltpu.VMEM(column_taps.shape, BF16),
            pltpu.VMEM(interp.shape[::-1], BF16),
            pltpu.VMEM((tall, strip), BF16),
            pltpu.VMEM((tall, LANES), BF16),
            pltpu.VMEM((tall, LANES), BF16),
            pltpu.VMEM((height, 2 * LANES), BF16),
            pltpu.VMEM((height, strip), BF16),
            pltpu.VMEM((NK, UNIT, 2 * LANES), BF16),
            pltpu.VMEM((NK // 2, 2 * LANES, 2 * LANES), BF16),
            pltpu.VMEM((NK // 2, 2 * LANES, 2 * LANES), BF16),
            pltpu.VMEM((count, BLK, 2 * LANES), BF16),
            pltpu.VMEM((count, 2 * LANES, LANES), BF16),
            pltpu.VMEM((count, 2 * LANES, LANES), BF16),
            pltpu.VMEM((NK, tall, wide), BF16),
            pltpu.VMEM((height + 2 * EDGE, wide), BF16),
            pltpu.VMEM((height, wide), BF16),
            pltpu.VMEM((height + 16, strip), F32),
            pltpu.VMEM((16, LANES), F32),
            pltpu.VMEM((2, LANES), F32),
            pltpu.VMEM((n, 2, LANES), F32),
            pltpu.SemaphoreType.DMA((slots, 2)),
            pltpu.SemaphoreType.DMA((slots, 2)),
            pltpu.SemaphoreType.DMA((2,)),
            pltpu.SemaphoreType.DMA((2,)),
            pltpu.SemaphoreType.DMA((2,)),
            pltpu.SemaphoreType.DMA,
            pltpu.SemaphoreType.DMA,
            pltpu.SemaphoreType.DMA,
            pltpu.SemaphoreType.DMA,
            pltpu.SemaphoreType.REGULAR,
            pltpu.SemaphoreType.REGULAR,
            pltpu.SemaphoreType.DMA((9,)),
        ],
        compiler_params=pltpu.CompilerParams(
            collective_id=0, has_side_effects=True, vmem_limit_bytes=48 * 1024 * 1024
        ),
    )(
        pin(kernel_weight),
        pin(jnp.transpose(block_shift, (0, 2, 1))),
        pin(jnp.transpose(block_phase, (0, 2, 1))),
        pin(care.T),
        pin(design),
        pin(row_taps),
        pin(column_taps),
        pin(interp.T),
        pin(image),
    )
    return pl.pallas_call(
        normalize,
        out_shape=jax.ShapeDtypeStruct((height, strip), BF16),
        in_specs=[vmem] * 3,
        out_specs=hbm,
        scratch_shapes=[
            pltpu.VMEM((height, strip), BF16),
            pltpu.SemaphoreType.DMA((height // PIECE,)),
        ],
        compiler_params=pltpu.CompilerParams(vmem_limit_bytes=8 * 1024 * 1024),
    )(filtered, mean, scale)


def solution(mesh):
    placed = (
        P(("swath", "band"), None),
        P(),
        P(),
        P(),
        P(),
        P(None, "swath", "band"),
        P(None, "swath", "band"),
        P("swath", "band"),
        P("swath", "band"),
    )
    return jax.shard_map(
        on_device, mesh=mesh, in_specs=placed, out_specs=P("swath", "band"), check_vma=False
    )
```
